32 devices in a mesh: ctx: 16 (over z, y, core), tp: 2 (over x).
Axes of the slice: x: 2, y: 2, z: 4, core: 2. Of those that a mesh axis runs over, the one named last changes fastest.
Arguments:
- query_se: bfloat16 [3584, 8192], P('ctx', 'tp'), may hold values from -6 to 6
- key_se: bfloat16 [3584, 8192], P('ctx', 'tp'), may hold values from -6 to 6
- value_se: bfloat16 [3584, 8192], P('ctx', 'tp'), may hold values from -6 to 6
- query_mr: bfloat16 [3584, 8192], P('ctx', 'tp'), may hold values from -6 to 6
- key_mr: bfloat16 [3584, 8192], P('ctx', 'tp'), may hold values from -6 to 6
- upstream: bfloat16 [3584, 8192], P('ctx', 'tp'), may hold values from -6 to 6
- filter_se: float32 [7, 8192], P(None, 'tp'), may hold values from -2 to 2
- filter_mr: float32 [128, 8192], P(None, 'tp'), may hold values from -0.5 to 0.5
- skip_mr: float32 [8192], P('tp'), may hold values from -1 to 1
- norm_gain: float32 [8192], P('tp'), may hold values from 0.1 to 1.9
Outputs:
- grad_query_se: bfloat16 [3584, 8192], P('ctx', 'tp')
- grad_key_se: bfloat16 [3584, 8192], P('ctx', 'tp')
- grad_value_se: bfloat16 [3584, 8192], P('ctx', 'tp')
- grad_query_mr: bfloat16 [3584, 8192], P('ctx', 'tp')
- grad_key_mr: bfloat16 [3584, 8192], P('ctx', 'tp')
- grad_filter_se: float32 [7, 8192], P(None, ('tp', 'ctx'))
- grad_filter_mr: float32 [128, 8192], P(None, ('tp', 'ctx'))
- grad_skip: float32 [8192], P(('tp', 'ctx'))
- grad_gain: float32 [8192], P(('tp', 'ctx'))
The draws below stay inside these ranges and needn't reach their ends.
All inputs are finite; a program needn't handle non-finite values.
Results may differ from the reference program's by a relative error of at most 0.0062.
Values may be sent and summed in bfloat16 or wider, within the bound.
A program may use at most 128 MiB of HBM per device.

```python
import math
import jax
import jax.numpy as jnp
from jax import lax

D = 8192
SE_TAPS = 7
MR_TAPS = 128
TOKENS = 3584


def block_scale(rng, dims, split, least, high):
    loudness, own = 1.0, jax.random.fold_in(rng, 6)
    for dim, blocks in split:
        heights = jnp.exp(jax.random.uniform(jax.random.fold_in(own, dim), (blocks,), jnp.float32, least / len(split), high / len(split)))
        loudness = loudness * jnp.repeat(heights, dims[dim] // blocks).reshape([-1 if axis == dim else 1 for axis in range(len(dims))])
    return loudness


def bell_draw(key, extent, scale, limit, pieces=(), kind=jnp.bfloat16):
    loudness = block_scale(key, extent, pieces, -0.22, 0.18) if pieces else 1.0
    drawn = jax.random.normal(key, extent, jnp.float32) * scale * loudness
    return jnp.minimum(jnp.maximum(drawn, -limit), limit).astype(kind)


def setup_inputs(seed: int = 0) -> dict:
    streams_of = jax.random.split(jax.random.key(seed), 11)
    query_se = bell_draw(streams_of[0], (TOKENS, D), 1.0, 6.0, ((0, 16), (1, 2)))
    key_se = bell_draw(streams_of[1], (TOKENS, D), 1.0, 6.0, ((0, 16), (1, 2)))
    value_se = bell_draw(streams_of[2], (TOKENS, D), 1.0, 6.0, ((0, 16), (1, 2)))
    query_mr = bell_draw(streams_of[3], (TOKENS, D), 1.0, 6.0, ((0, 16), (1, 2)))
    key_mr = bell_draw(streams_of[4], (TOKENS, D), 1.0, 6.0, ((0, 16), (1, 2)))
    upstream = bell_draw(streams_of[5], (TOKENS, D), 1.0, 6.0, ((0, 16), (1, 2)))
    filter_se = bell_draw(streams_of[6], (SE_TAPS, D), SE_TAPS ** -0.5, 2.0, ((1, 2),), jnp.float32)
    filter_mr = bell_draw(streams_of[7], (MR_TAPS, D), MR_TAPS ** -0.5, 0.5, ((1, 2),), jnp.float32)
    skip_mr = jnp.clip(jax.random.uniform(streams_of[8], (D,), jnp.float32, -1.0, 1.0) * block_scale(streams_of[8], (D,), ((0, 2),), -0.4, 0.0), -1.0, 1.0)
    norm_gain = jnp.clip(1.0 + 0.18 * jax.random.normal(streams_of[9], (D,), jnp.float32), 0.1, 1.9)
    return {"query_se": query_se, "key_se": key_se, "value_se": value_se, "query_mr": query_mr, "key_mr": key_mr, "upstream": upstream, "filter_se": filter_se, "filter_mr": filter_mr, "skip_mr": skip_mr, "norm_gain": norm_gain}


EPSILON = 0.1

def rounded(value):
    half = lax.optimization_barrier(value.astype(jnp.bfloat16))
    return half.astype(jnp.float32)

def to_blocks(array, width):
    rows, chans = array.shape
    return array.reshape(rows, chans // width, width).transpose(1, 0, 2)

def from_blocks(array):
    count, rows, width = array.shape
    return array.transpose(1, 0, 2).reshape(rows, count * width)

def shift_down(field, steps):
    zeros = jnp.zeros((steps, field.shape[1]), field.dtype)
    return jnp.concatenate([zeros, field[:field.shape[0] - steps]], 0)

def shift_up(field, steps):
    zeros = jnp.zeros((steps, field.shape[1]), field.dtype)
    return jnp.concatenate([field[steps:], zeros], 0)

def short_conv(field, taps):
    result = taps[0] * field
    for step in range(1, taps.shape[0]):
        result = result + taps[step] * shift_down(field, step)
    return result

def short_adjoint(field, taps):
    result = taps[0] * field
    for step in range(1, taps.shape[0]):
        result = result + taps[step] * shift_up(field, step)
    return result

def short_corr(grads, field, count):
    return jnp.stack([lax.optimization_barrier(jnp.sum(grads * shift_down(field, step), axis=0)) for step in range(count)], 0)

def long_conv(field, taps, length):
    spectrum = jnp.fft.rfft(field, n=length, axis=0) * jnp.fft.rfft(taps, n=length, axis=0)
    return jnp.fft.irfft(spectrum, n=length, axis=0)[:field.shape[0]]

def long_adjoint(field, taps, length):
    spectrum = jnp.fft.rfft(field, n=length, axis=0) * jnp.conj(jnp.fft.rfft(taps, n=length, axis=0))
    return jnp.fft.irfft(spectrum, n=length, axis=0)[:field.shape[0]]

def long_corr(grads, field, length, count):
    spectrum = jnp.fft.rfft(grads, n=length, axis=0) * jnp.conj(jnp.fft.rfft(field, n=length, axis=0))
    return jnp.fft.irfft(spectrum, n=length, axis=0)[:count]

def reference(query_se, key_se, value_se, query_mr, key_mr, upstream, filter_se, filter_mr, skip_mr, norm_gain):
    width = math.gcd(D, 1024)
    count = D // width
    length = TOKENS + MR_TAPS
    b_qse = to_blocks(query_se, width)
    b_kse = to_blocks(key_se, width)
    b_vse = to_blocks(value_se, width)
    b_qmr = to_blocks(query_mr, width)
    b_kmr = to_blocks(key_mr, width)
    b_up = to_blocks(upstream, width)
    b_fse = to_blocks(filter_se, width)
    b_fmr = to_blocks(filter_mr, width)
    b_skip = skip_mr.reshape(count, width)
    b_gain = norm_gain.reshape(count, width)

    def short_layer(query, keys, values, taps):
        product = rounded(keys.astype(jnp.float32) * values.astype(jnp.float32))
        conv = short_conv(product, taps)
        return (product, conv, query.astype(jnp.float32) * conv)

    def first(items):
        query, keys, values, taps = items
        product, conv, mixed = short_layer(query, keys, values, taps)
        return lax.optimization_barrier(jnp.sum(mixed * mixed, axis=1))
    squares = lax.optimization_barrier(jnp.sum(lax.map(first, (b_qse, b_kse, b_vse, b_fse)), axis=0))
    scale_rows = lax.rsqrt(squares / D + EPSILON)

    def second(items):
        query, keys, values, taps, gate_q, gate_k, cotan, long_taps, skip, gain = items
        product, conv, mixed = short_layer(query, keys, values, taps)
        normed = mixed * scale_rows[:, None] * gain
        product_mr = rounded(gate_k.astype(jnp.float32) * normed)
        conv_mr = long_conv(product_mr, long_taps, length) + skip * product_mr
        cot = cotan.astype(jnp.float32)
        grad_query_mr = (cot * conv_mr).astype(jnp.bfloat16)
        grad_conv_mr = rounded(cot * gate_q.astype(jnp.float32))
        grad_product_mr = long_adjoint(grad_conv_mr, long_taps, length) + skip * grad_conv_mr
        grad_key_mr = (grad_product_mr * normed).astype(jnp.bfloat16)
        grad_normed = grad_product_mr * gate_k.astype(jnp.float32)
        weighted = lax.optimization_barrier(jnp.sum(grad_normed * gain * mixed, axis=1))
        grad_filter_mr = long_corr(grad_conv_mr, product_mr, length, MR_TAPS)
        grad_skip = lax.optimization_barrier(jnp.sum(grad_conv_mr * product_mr, axis=0))
        grad_gain = lax.optimization_barrier(jnp.sum(grad_normed * mixed * scale_rows[:, None], axis=0))
        return (grad_query_mr, grad_key_mr, grad_normed, weighted, grad_filter_mr, grad_skip, grad_gain)
    out_b = lax.map(second, (b_qse, b_kse, b_vse, b_fse, b_qmr, b_kmr, b_up, b_fmr, b_skip, b_gain))
    grad_query_mr, grad_key_mr, grad_normed, weighted, grad_filter_mr, grad_skip, grad_gain = out_b
    weighted = lax.optimization_barrier(jnp.sum(weighted, axis=0))

    def third(items):
        query, keys, values, taps, gain, back = items
        product, conv, mixed = short_layer(query, keys, values, taps)
        grad_mixed = gain * scale_rows[:, None] * back - mixed * (scale_rows ** 3 * weighted / D)[:, None]
        grad_query_se = (grad_mixed * conv).astype(jnp.bfloat16)
        grad_conv_se = rounded(grad_mixed * query.astype(jnp.float32))
        grad_product_se = short_adjoint(grad_conv_se, taps)
        grad_key_se = (grad_product_se * values.astype(jnp.float32)).astype(jnp.bfloat16)
        grad_value_se = (grad_product_se * keys.astype(jnp.float32)).astype(jnp.bfloat16)
        grad_filter_se = short_corr(grad_conv_se, product, SE_TAPS)
        return (grad_query_se, grad_key_se, grad_value_se, grad_filter_se)
    grad_query_se, grad_key_se, grad_value_se, grad_filter_se = lax.map(third, (b_qse, b_kse, b_vse, b_fse, b_gain, grad_normed))
    factor = 1.0 / math.sqrt(TOKENS)
    return (from_blocks(grad_query_se), from_blocks(grad_key_se), from_blocks(grad_value_se), from_blocks(grad_query_mr), from_blocks(grad_key_mr), from_blocks(grad_filter_se) * factor, from_blocks(grad_filter_mr) * factor, grad_skip.reshape(D) * factor, grad_gain.reshape(D) * factor)
```

```python
import functools
import math

import jax
import jax.numpy as jnp
import numpy as np
from jax import lax
from jax.experimental import pallas as pl
from jax.experimental.pallas import tpu as pltpu
from jax.sharding import PartitionSpec as P

EPSILON = 0.1
F32 = jnp.float32
BF16 = jnp.bfloat16
LANES = 128
MESH = pl.DeviceIdType.MESH


def transforms(rows, taps):
    length = rows + taps
    freq = 2.0 * np.pi * (np.arange(length // 2) + 0.5) / length

    def forward(start, stop):
        angle = freq[:, None] * np.arange(start, stop)[None, :]
        return np.concatenate([np.cos(angle), -np.sin(angle)], 0)

    angle = np.arange(max(rows, taps))[:, None] * freq[None, :]
    inverse = np.concatenate([np.cos(angle), -np.sin(angle)], 1) * (2.0 / length)
    mats = forward(-taps, rows), forward(0, length), inverse
    return [jnp.asarray(m, BF16) for m in mats]


def dot(a, b):
    return jnp.dot(a, b, preferred_element_type=F32)


def spectrum_of(real, imag):
    return jnp.concatenate([real.astype(BF16), imag.astype(BF16)], 0)


def up_to(value, step):
    return -(-value // step) * step


def layer_kernel(width, nctx, ntp, *refs):
    (q_h, k_h, v_h, qm_h, km_h, up_h, fse_h, fmr_h, skip_h, gain_h, fg_h, fz_h, inv_h,
     gq_o, gk_o, gv_o, gqm_o, gkm_o, corr_o, small_o,
     q, k, v, qm, km, up, fse, fmr, skip, gain, fg, fz, inv,
     ends, tail_out, tail_in, head_out, head_in,
     gfull, zfull, conv, normed, gn, hs, zs, prod, pad_g, corr, small,
     acc, scale, coef, row_out, row_in,
     in_sem, small_sem, out_sem, edge_send, edge_recv, head_send, head_recv, tail_send, tail_recv,
     row_send, row_recv) = refs
    nblk, rows, blk = q.shape
    taps_se, taps = fse.shape[1], fmr.shape[1]
    halo = tail_in.shape[0]
    half = fg.shape[0] // 2
    parts, _, group = corr.shape
    ppb = parts // nblk
    cpb = blk // LANES
    ctx, tp = lax.axis_index("ctx"), lax.axis_index("tp")
    first, last = ctx == 0, ctx == nctx - 1

    def cols_of(c):
        return pl.ds(pl.multiple_of(c * blk, blk), blk)

    def local(src, dst, sem):
        return pltpu.make_async_copy(src, dst, sem)

    def remote(src, dst, send, recv, where):
        return pltpu.make_async_remote_copy(
            src_ref=src, dst_ref=dst, send_sem=send, recv_sem=recv,
            device_id=where, device_id_type=MESH,
        )

    streams = ((up_h, up), (qm_h, qm), (k_h, k), (v_h, v), (q_h, q), (km_h, km), (fmr_h, fmr))

    def load(s, c):
        src, dst = streams[s]
        return local(src.at[:, cols_of(c)], dst.at[c], in_sem.at[s, c])

    def wide(s, c):
        src, dst = ((fse_h, fse), (skip_h, skip), (gain_h, gain))[s]
        return local(src.at[:, cols_of(c)], dst.at[c], small_sem.at[s, c])

    def whole(s):
        src, dst = ((fg_h, fg), (fz_h, fz), (inv_h, inv))[s]
        return local(src, dst, edge_send.at[2 + s])

    end_k = local(k_h.at[pl.ds(rows - halo, halo), :], ends.at[0], edge_send.at[5])
    end_v = local(v_h.at[pl.ds(rows - halo, halo), :], ends.at[1], edge_send.at[6])
    end_k.start()
    end_v.start()

    def start(*which):
        def step(c, carry):
            for s in which:
                load(s, c).start()
            return carry
        lax.fori_loop(0, nblk, step, 0)

    start(0, 1)

    def start_wide(c, carry):
        for s in range(3):
            wide(s, c).start()
        return carry

    lax.fori_loop(0, nblk, start_wide, 0)
    start(2, 3, 4)
    for s in range(3):
        whole(s).start()
    start(6)
    start(5)

    barrier = pltpu.get_barrier_semaphore()

    def greet(**where):
        pl.semaphore_signal(barrier, inc=1, device_id=where, device_id_type=MESH)

    before, after = {"ctx": ctx - 1}, {"ctx": ctx + 1}
    pl.when(ctx > 0)(lambda: greet(ctx=ctx - 1))
    pl.when(ctx < nctx - 1)(lambda: greet(ctx=ctx + 1))
    for step in range(1, ntp):
        greet(tp=lax.rem(tp + step, ntp))
    pl.semaphore_wait(
        barrier, ntp - 1 + (ctx > 0).astype(jnp.int32) + (ctx < nctx - 1).astype(jnp.int32)
    )

    tail_se = remote(tail_out, tail_in, edge_send.at[0], edge_recv.at[0], after)
    head_se = remote(head_out, head_in, edge_send.at[1], edge_recv.at[1], before)

    def head_mr(c):
        return remote(gfull.at[c, pl.ds(0, taps), :], gfull.at[c, pl.ds(rows, taps), :],
                      head_send.at[c], head_recv.at[c], before)

    def tail_mr(c):
        return remote(zfull.at[c, pl.ds(rows, taps), :], zfull.at[c, pl.ds(0, taps), :],
                      tail_send.at[c], tail_recv.at[c], after)

    end_k.wait()
    end_v.wait()
    tail_out[...] = (ends[0].astype(F32) * ends[1].astype(F32)).astype(BF16)
    pl.when(ctx < nctx - 1)(tail_se.start)

    @pl.when(first)
    def _():
        tail_in[...] = jnp.zeros_like(tail_in)
        zfull[:, :taps, :] = jnp.zeros((nblk, taps, blk), BF16)

    @pl.when(last)
    def _():
        head_in[...] = jnp.zeros_like(head_in)
        gfull[:, rows:, :] = jnp.zeros((nblk, taps, blk), BF16)

    def gate_step(c, carry):
        load(0, c).wait()
        load(1, c).wait()
        gfull[c, :rows, :] = (up[c].astype(F32) * qm[c].astype(F32)).astype(BF16)
        pl.when(ctx > 0)(lambda: head_mr(c).start())
        return carry

    lax.fori_loop(0, nblk, gate_step, 0)

    acc[...] = jnp.zeros_like(acc)
    pl.when(ctx > 0)(tail_se.wait_recv)

    def short_step(c, carry):
        for s in range(3):
            wide(s, c).wait()
            load(2 + s, c).wait()
        for i in range(cpb):
            cols = slice(i * LANES, (i + 1) * LANES)
            lane = c * cpb + i
            at = pl.ds(pl.multiple_of(lane * LANES, LANES), LANES)
            prod[lane, :halo, :] = tail_in[:, at].astype(F32)
            product = k[c, :, cols].astype(F32) * v[c, :, cols].astype(F32)
            prod[lane, halo:, :] = product.astype(BF16).astype(F32)
            out = fse[c, 0:1, cols] * prod[lane, pl.ds(halo, rows), :]
            for j in range(1, taps_se):
                out = out + fse[c, j : j + 1, cols] * prod[lane, pl.ds(halo - j, rows), :]
            conv[c, :, cols] = out
            mixed = q[c, :, cols].astype(F32) * out
            acc[:rows, :] += mixed * mixed
        return carry

    lax.fori_loop(0, nblk, short_step, 0)

    def row_copy(which, step):
        return remote(row_out.at[which], row_in.at[which, step - 1],
                      row_send.at[which, step - 1], row_recv.at[which, step - 1],
                      {"tp": lax.rem(tp + step, ntp)})

    def send_rows(which):
        total = jnp.sum(jnp.transpose(acc[...]), axis=0, keepdims=True)
        row_out[which] = jnp.broadcast_to(total, row_out.shape[1:])
        for step in range(1, ntp):
            row_copy(which, step).start()

    def sum_rows(which):
        total = row_out[which]
        for step in range(1, ntp):
            row_copy(which, step).wait_recv()
            total = total + row_in[which, step - 1]
        return total[0:1, :]

    def as_column(line):
        return jnp.transpose(jnp.broadcast_to(line, (LANES, line.shape[1])))[:rows, :]

    send_rows(0)

    for s in range(3):
        whole(s).wait()

    def filter_step(c, carry):
        load(6, c).wait()
        spec = dot(fz[:, taps : 2 * taps], fmr[c].astype(BF16))
        hs[c, :half, :] = spec[:half] + skip[c]
        hs[c, half:, :] = spec[half:]
        return carry

    lax.fori_loop(0, nblk, filter_step, 0)

    scale[...] = as_column(lax.rsqrt(sum_rows(0) * (1.0 / width) + EPSILON))

    def product_step(c, carry):
        load(5, c).wait()
        for i in range(cpb):
            cols = slice(i * LANES, (i + 1) * LANES)
            mixed = q[c, :, cols].astype(F32) * conv[c, :, cols]
            value = mixed * scale[...] * gain[c, :, cols]
            normed[c, :, cols] = value
            zfull[c, taps:, cols] = (km[c, :, cols].astype(F32) * value).astype(BF16)
        pl.when(ctx < nctx - 1)(lambda: tail_mr(c).start())
        return carry

    lax.fori_loop(0, nblk, product_step, 0)

    acc[...] = jnp.zeros_like(acc)

    def adjoint_step(c, carry):
        pl.when(ctx < nctx - 1)(lambda: head_mr(c).wait_recv())
        gs = dot(fg[...], gfull[c])
        gr, gi = gs[:half], gs[half:]
        hr, hi = hs[c, :half, :], hs[c, half:, :]
        gp = dot(inv[:rows, :], spectrum_of(gr * hr + gi * hi, gi * hr - gr * hi))
        for i in range(cpb):
            cols = slice(i * LANES, (i + 1) * LANES)
            back, value = gp[:, cols], normed[c, :, cols]
            grad = back * km[c, :, cols].astype(F32)
            qm[c, :, cols] = (back * value).astype(BF16)
            gn[c, :, cols] = grad
            acc[:rows, :] += grad * value
        local(qm.at[c], gkm_o.at[:, cols_of(c)], out_sem.at[0, c]).start()
        spec = dot(fz[:, taps:], zfull[c, taps:, :])
        zs[c] = spec
        zr, zi = spec[:half], spec[half:]
        part = dot(inv[:taps, :], spectrum_of(gr * zr + gi * zi, gi * zr - gr * zi))
        for p in range(ppb):
            corr[c * ppb + p] = part[:, p * group : (p + 1) * group]
        return carry

    lax.fori_loop(0, nblk, adjoint_step, 0)
    corr_copy = local(corr, corr_o, out_sem.at[5, 0])
    corr_copy.start()

    send_rows(1)

    def medium_step(c, carry):
        pl.when(ctx > 0)(lambda: tail_mr(c).wait_recv())
        spec = zs[c] + dot(fz[:, :taps], zfull[c, :taps, :])
        zr, zi = spec[:half], spec[half:]
        hr, hi = hs[c, :half, :], hs[c, half:, :]
        out = dot(inv[:rows, :], spectrum_of(zr * hr - zi * hi, zr * hi + zi * hr))
        up[c] = (up[c].astype(F32) * out).astype(BF16)
        local(up.at[c], gqm_o.at[:, cols_of(c)], out_sem.at[1, c]).start()
        return carry

    lax.fori_loop(0, nblk // 2, medium_step, 0)

    weight = as_column(sum_rows(1))
    coef[...] = weight * (scale[...] * scale[...]) * (1.0 / width)

    def grad_mixed(c, cols, top):
        at = slice(0, top)
        back = gn[c, at, cols] * scale[at, :]
        quer = q[c, at, cols].astype(F32)
        mixed = quer * conv[c, at, cols]
        return back, quer, mixed, gain[c, :, cols] * back - mixed * coef[at, :]

    def edge_step(c, carry):
        for i in range(cpb):
            cols = slice(i * LANES, (i + 1) * LANES)
            at = pl.ds(pl.multiple_of(c * blk + i * LANES, LANES), LANES)
            _, quer, _, gm = grad_mixed(c, cols, halo)
            head_out[:, at] = (gm * quer).astype(BF16)
        return carry

    lax.fori_loop(0, nblk, edge_step, 0)
    pl.when(ctx > 0)(head_se.start)

    lax.fori_loop(nblk // 2, nblk, medium_step, 0)

    pl.when(ctx < nctx - 1)(head_se.wait_recv)

    def back_step(c, carry):
        for i in range(cpb):
            cols = slice(i * LANES, (i + 1) * LANES)
            lane = c * cpb + i
            at = pl.ds(pl.multiple_of(lane * LANES, LANES), LANES)
            back, quer, mixed, gm = grad_mixed(c, cols, rows)
            gc = (gm * quer).astype(BF16).astype(F32)
            pad_g[i, :rows, :] = gc
            pad_g[i, rows:, :] = head_in[:, at].astype(F32)
            part, inner = i * LANES // group, i * LANES % group
            place = slice(inner, inner + LANES)
            small[c * ppb + part, taps_se : taps_se + 1, place] = jnp.sum(
                back * mixed, axis=0, keepdims=True
            )
            q[c, :, cols] = (gm * conv[c, :, cols]).astype(BF16)
            gp = fse[c, 0:1, cols] * gc
            for j in range(taps_se):
                if j:
                    gp = gp + fse[c, j : j + 1, cols] * pad_g[i, pl.ds(j, rows), :]
                small[c * ppb + part, j : j + 1, place] = jnp.sum(
                    gc * prod[lane, pl.ds(halo - j, rows), :], axis=0, keepdims=True
                )
            key = k[c, :, cols].astype(F32)
            k[c, :, cols] = (gp * v[c, :, cols].astype(F32)).astype(BF16)
            v[c, :, cols] = (gp * key).astype(BF16)
        for s, (src, dst) in enumerate(((q, gq_o), (k, gk_o), (v, gv_o))):
            local(src.at[c], dst.at[:, cols_of(c)], out_sem.at[2 + s, c]).start()
        return carry

    lax.fori_loop(0, nblk, back_step, 0)
    small_copy = local(small, small_o, out_sem.at[5, 1])
    small_copy.start()

    def finish(c, carry):
        pairs = ((qm, gkm_o), (up, gqm_o), (q, gq_o), (k, gk_o), (v, gv_o))
        for s, (src, dst) in enumerate(pairs):
            local(src.at[c], dst.at[:, cols_of(c)], out_sem.at[s, c]).wait()
        pl.when(ctx > 0)(lambda: head_mr(c).wait_send())
        pl.when(ctx < nctx - 1)(lambda: tail_mr(c).wait_send())
        return carry

    lax.fori_loop(0, nblk, finish, 0)
    corr_copy.wait()
    small_copy.wait()
    pl.when(ctx < nctx - 1)(tail_se.wait_send)
    pl.when(ctx > 0)(head_se.wait_send)
    for which in range(2):
        for step in range(1, ntp):
            row_copy(which, step).wait_send()


def split_parts(parts, share):
    count, height, group = parts.shape
    if group == share:
        return parts
    parts = parts.reshape(count, height, group // share, share)
    return parts.transpose(0, 2, 1, 3).reshape(-1, height, share)


def scatter_sum(parts, axis):
    size = lax.axis_size(axis)
    me = lax.axis_index(axis)
    bit = 1
    while bit < size:
        rest = parts.reshape((parts.shape[0] // 2, 2) + parts.shape[1:])
        mine = lax.rem(me // bit, 2)
        away = lax.dynamic_index_in_dim(rest, 1 - mine, 1, keepdims=False).astype(BF16)
        keep = lax.dynamic_index_in_dim(rest, mine, 1, keepdims=False)
        with jax.named_scope(f"halve_{bit}"):
            got = lax.ppermute(away, axis, [(i, i ^ bit) for i in range(size)])
        parts = keep + got.astype(F32)
        bit *= 2
    return parts[0]


def local(
    query_se, key_se, value_se, query_mr, key_mr, upstream, filter_se, filter_mr, skip_mr, norm_gain
):
    rows, chans = query_se.shape
    taps_se, taps = filter_se.shape[0], filter_mr.shape[0]
    ctx, ntp = lax.axis_size("ctx"), lax.axis_size("tp")
    width = chans * ntp
    tokens = rows * ctx
    share = chans // ctx
    group = up_to(share, LANES)
    halo = up_to(taps_se - 1, 16)
    blk = max(group, min(512, chans))
    nblk = chans // blk
    fz, fg, inv = transforms(rows, taps)
    length = rows + taps
    tall = up_to(rows, LANES)
    nlane = chans // LANES

    def out(shape, kind):
        return jax.ShapeDtypeStruct(shape, kind)

    ins = (query_se, key_se, value_se, query_mr, key_mr, upstream, filter_se, filter_mr,
           skip_mr[None], norm_gain[None], fg, fz, inv)
    outs = [out((rows, chans), BF16)] * 5 + [
        out((chans // group, taps, group), F32), out((chans // group, taps_se + 1, group), F32)
    ]
    V, D = pltpu.VMEM, pltpu.SemaphoreType.DMA
    stream = V((nblk, rows, blk), BF16)
    scratch = [stream] * 6 + [
        V((nblk, taps_se, blk), F32), V((nblk, taps, blk), F32), V((nblk, 1, blk), F32),
        V((nblk, 1, blk), F32), V(fg.shape, BF16), V(fz.shape, BF16), V(inv.shape, BF16),
        V((2, halo, chans), BF16), V((halo, chans), BF16), V((halo, chans), BF16),
        V((halo, chans), BF16), V((halo, chans), BF16),
        V((nblk, length, blk), BF16), V((nblk, length, blk), BF16),
        V((nblk, rows, blk), F32), V((nblk, rows, blk), F32), V((nblk, rows, blk), F32),
        V((nblk, length, blk), F32), V((nblk, length, blk), F32),
        V((nlane, halo + rows, LANES), F32), V((blk // LANES, halo + rows, LANES), F32),
        V(outs[5].shape, F32), V(outs[6].shape, F32),
        V((tall, LANES), F32), V((rows, LANES), F32), V((rows, LANES), F32),
        V((2, 8, tall), F32), V((2, max(ntp - 1, 1), 8, tall), F32),
        D((7, nblk)), D((3, nblk)), D((6, max(nblk, 2))), D((7,)), D((2,)),
        D((nblk,)), D((nblk,)), D((nblk,)), D((nblk,)),
        D((2, max(ntp - 1, 1))), D((2, max(ntp - 1, 1))),
    ]
    anywhere = pl.BlockSpec(memory_space=pl.ANY)
    with jax.named_scope("layer"):
        (grad_query_se, grad_key_se, grad_value_se, grad_query_mr, grad_key_mr, corr,
         small) = pl.pallas_call(
            functools.partial(layer_kernel, width, ctx, ntp),
            name="layer",
            in_specs=[anywhere] * len(ins),
            out_specs=[anywhere] * len(outs),
            out_shape=outs,
            scratch_shapes=scratch,
            compiler_params=pltpu.CompilerParams(
                collective_id=0, has_side_effects=True, vmem_limit_bytes=62 * 2**20
            ),
        )(*ins)
    corr, small = split_parts(corr, share), split_parts(small, share)
    small = lax.all_to_all(small, "ctx", 0, 0, tiled=True)
    factor = 1.0 / math.sqrt(tokens)
    total_mr = scatter_sum(corr, "ctx") * factor
    total = jnp.sum(small, axis=0) * factor
    return (
        grad_query_se,
        grad_key_se,
        grad_value_se,
        grad_query_mr,
        grad_key_mr,
        total[:taps_se],
        total_mr,
        total_mr[0],
        total[taps_se],
    )


def solution(mesh):
    streams = (P("ctx", "tp"),)
    in_specs = streams * 6 + (P(None, "tp"), P(None, "tp"), P("tp"), P("tp"))
    both = ("tp", "ctx")
    out_specs = streams * 5 + (P(None, both), P(None, both), P(both), P(both))
    return jax.shard_map(local, mesh=mesh, in_specs=in_specs, out_specs=out_specs, check_vma=False)
```

```python
import functools
import math

import jax
import jax.numpy as jnp
import numpy as np
from jax import lax
from jax.experimental import pallas as pl
from jax.experimental.pallas import tpu as pltpu
from jax.sharding import PartitionSpec as P

EPSILON = 0.1
F32 = jnp.float32
BF16 = jnp.bfloat16
LANES = 128
MESH = pl.DeviceIdType.MESH


def transforms(rows, taps):
    length = rows + taps
    freq = 2.0 * np.pi * (np.arange(length // 2) + 0.5) / length

    def forward(start, stop):
        angle = freq[:, None] * np.arange(start, stop)[None, :]
        return np.concatenate([np.cos(angle), -np.sin(angle)], 0)

    angle = np.arange(max(rows, taps))[:, None] * freq[None, :]
    inverse = np.concatenate([np.cos(angle), -np.sin(angle)], 1) * (2.0 / length)
    mats = forward(-taps, rows), forward(0, length), inverse
    return [jnp.asarray(m, BF16) for m in mats]


def dot(a, b):
    return jnp.dot(a, b, preferred_element_type=F32)


def spectrum_of(real, imag):
    return jnp.concatenate([real.astype(BF16), imag.astype(BF16)], 0)


def up_to(value, step):
    return -(-value // step) * step


def halving_bits(size, ratio):
    bits = []
    bit = ratio
    while bit < size:
        bits.append(bit)
        bit *= 2
    return bits[:1] + bits[2:] + bits[1:2]


def runs(count):
    return 2 if count % 2 == 0 else 1


def layer_kernel(width, tokens, nctx, ntp, ratio, *refs):
    (q_h, k_h, v_h, qm_h, km_h, up_h, fse_h, fmr_h, skip_h, gain_h, fg_h, fz_h, inv_h,
     q, k, v, qm, up, total_o, small_o,
     km, fse, fmr, skip, gain, fg, fz, inv, ends, tail_out, tail_in, head_out, head_in,
     gfull, zfull, conv, normed, hs, zs, prod, pad_g, corr, small, away, got, small_in,
     acc, scale, coef, row_out, row_in,
     in_sem, small_sem, edge_sem, edge_send, edge_recv, head_send, head_recv, tail_send, tail_recv,
     row_send, row_recv, halve_send, halve_recv, swap_send, swap_recv) = refs
    nblk, rows, blk = q.shape
    taps_se, taps = fse.shape[1], fmr.shape[1]
    halo = tail_in.shape[0]
    half = fg.shape[0] // 2
    parts, _, group = corr.shape
    ppb = parts // nblk
    cpb = blk // LANES
    ctx, tp = lax.axis_index("ctx"), lax.axis_index("tp")
    first, last = ctx == 0, ctx == nctx - 1
    bits = halving_bits(nctx, ratio)
    factor = 1.0 / math.sqrt(tokens)

    def cols_of(c):
        return pl.ds(pl.multiple_of(c * blk, blk), blk)

    def each(count, body, start=0):
        def step(c, carry):
            body(c)
            return carry
        lax.fori_loop(start, start + count, step, 0)

    def several(start, stop, body):
        n = runs(stop - start)
        each((stop - start) // n, lambda p: body([start + p * n + u for u in range(n)]))

    def remote(src, dst, send, recv, where):
        return pltpu.make_async_remote_copy(
            src_ref=src, dst_ref=dst, send_sem=send, recv_sem=recv,
            device_id=where, device_id_type=MESH,
        )

    streams = ((up_h, up), (qm_h, qm), (k_h, k), (v_h, v), (q_h, q), (km_h, km), (fmr_h, fmr))

    def load(s, c):
        src, dst = streams[s]
        return pltpu.make_async_copy(src.at[:, cols_of(c)], dst.at[c], in_sem.at[s, c])

    def wide(s, c):
        src, dst = ((fse_h, fse), (skip_h, skip), (gain_h, gain))[s]
        return pltpu.make_async_copy(src.at[:, cols_of(c)], dst.at[c], small_sem.at[s, c])

    def single(s):
        bottom = pl.ds(rows - halo, halo)
        src, dst = ((k_h.at[bottom, :], ends.at[0]), (v_h.at[bottom, :], ends.at[1]),
                    (fg_h, fg), (fz_h, fz), (inv_h, inv))[s]
        return pltpu.make_async_copy(src, dst, edge_sem.at[s])

    barrier = pltpu.get_barrier_semaphore()
    for step in range(1, nctx):
        pl.semaphore_signal(barrier, inc=1, device_id={"ctx": lax.rem(ctx + step, nctx)},
                            device_id_type=MESH)
    for step in range(1, ntp):
        pl.semaphore_signal(barrier, inc=1, device_id={"tp": lax.rem(tp + step, ntp)},
                            device_id_type=MESH)

    def start_group(*which):
        def body(c):
            for s in which:
                load(s, c).start()
        each(nblk, body)

    def start_wide(c):
        for s in range(3):
            wide(s, c).start()

    single(0).start()
    single(1).start()
    start_group(0, 1)
    single(3).start()
    each(nblk, start_wide)
    start_group(6)
    start_group(2, 3, 4)
    single(2).start()
    single(4).start()
    start_group(5)

    @pl.when(first)
    def _():
        tail_in[...] = jnp.zeros_like(tail_in)
        zfull[:, :taps, :] = jnp.zeros((nblk, taps, blk), BF16)

    @pl.when(last)
    def _():
        head_in[...] = jnp.zeros_like(head_in)
        gfull[:, rows:, :] = jnp.zeros((nblk, taps, blk), BF16)

    before, after = {"ctx": ctx - 1}, {"ctx": ctx + 1}
    tail_se = remote(tail_out, tail_in, edge_send.at[0], edge_recv.at[0], after)
    head_se = remote(head_out, head_in, edge_send.at[1], edge_recv.at[1], before)

    def head_mr(c):
        return remote(gfull.at[c, pl.ds(0, taps), :], gfull.at[c, pl.ds(rows, taps), :],
                      head_send.at[c], head_recv.at[c], before)

    def tail_mr(c):
        return remote(zfull.at[c, pl.ds(rows, taps), :], zfull.at[c, pl.ds(0, taps), :],
                      tail_send.at[c], tail_recv.at[c], after)

    single(0).wait()
    single(1).wait()
    tail_out[...] = (ends[0].astype(F32) * ends[1].astype(F32)).astype(BF16)

    def gate_step(c):
        load(0, c).wait()
        load(1, c).wait()
        gfull[c, :rows, :] = (up[c].astype(F32) * qm[c].astype(F32)).astype(BF16)

    with jax.named_scope("p_gate"):
        each(nblk, gate_step)
    with jax.named_scope("p_bar"):
        pl.semaphore_wait(barrier, nctx + ntp - 2)
    pl.when(ctx < nctx - 1)(tail_se.start)
    single(3).wait()

    def filter_step(cs):
        for c in cs:
            load(6, c).wait()
            wide(1, c).wait()
        found = [dot(fz[:, taps : 2 * taps], fmr[c].astype(BF16)) for c in cs]
        for c, value in zip(cs, found):
            hs[c, :half, :] = value[:half] + skip[c]
            hs[c, half:, :] = value[half:]

    with jax.named_scope("p_filt1"):
        several(0, nblk // 2, filter_step)

    @pl.when(ctx > 0)
    def _():
        each(nblk, lambda c: head_mr(c).start())

    acc[...] = jnp.zeros_like(acc)
    with jax.named_scope("p_tailse"):
        pl.when(ctx > 0)(tail_se.wait_recv)

    def short_step(c):
        wide(0, c).wait()
        wide(2, c).wait()
        for s in range(3):
            load(2 + s, c).wait()
        for i in range(cpb):
            cols = slice(i * LANES, (i + 1) * LANES)
            lane = c * cpb + i
            at = pl.ds(pl.multiple_of(lane * LANES, LANES), LANES)
            prod[lane, :halo, :] = tail_in[:, at].astype(F32)
            product = k[c, :, cols].astype(F32) * v[c, :, cols].astype(F32)
            prod[lane, halo:, :] = product.astype(BF16).astype(F32)
            out = fse[c, 0:1, cols] * prod[lane, pl.ds(halo, rows), :]
            for j in range(1, taps_se):
                out = out + fse[c, j : j + 1, cols] * prod[lane, pl.ds(halo - j, rows), :]
            conv[c, :, cols] = out
            mixed = q[c, :, cols].astype(F32) * out
            acc[:rows, :] += mixed * mixed

    with jax.named_scope("p_short"):
        each(nblk, short_step)

    def row_copy(which, step):
        return remote(row_out.at[which], row_in.at[which, step - 1],
                      row_send.at[which, step - 1], row_recv.at[which, step - 1],
                      {"tp": lax.rem(tp + step, ntp)})

    def send_rows(which):
        total = jnp.sum(jnp.transpose(acc[...]), axis=0, keepdims=True)
        row_out[which] = jnp.broadcast_to(total, row_out.shape[1:])
        for step in range(1, ntp):
            row_copy(which, step).start()

    def sum_rows(which):
        total = row_out[which]
        for step in range(1, ntp):
            row_copy(which, step).wait_recv()
            total = total + row_in[which, step - 1]
        return total[0:1, :]

    def as_column(line):
        return jnp.transpose(jnp.broadcast_to(line, (LANES, line.shape[1])))[:rows, :]

    send_rows(0)
    with jax.named_scope("p_filt2"):
        several(nblk // 2, nblk, filter_step)
    acc[...] = jnp.zeros_like(acc)
    with jax.named_scope("p_scale"):
        scale[...] = as_column(lax.rsqrt(sum_rows(0) * (1.0 / width) + EPSILON))

    def product_step(c):
        load(5, c).wait()
        for i in range(cpb):
            cols = slice(i * LANES, (i + 1) * LANES)
            mixed = q[c, :, cols].astype(F32) * conv[c, :, cols]
            value = mixed * scale[...] * gain[c, :, cols]
            normed[c, :, cols] = value
            zfull[c, taps:, cols] = (km[c, :, cols].astype(F32) * value).astype(BF16)

    with jax.named_scope("p_prod"):
        each(nblk, product_step)

    single(2).wait()
    single(4).wait()

    def adjoint_step(cs):
        with jax.named_scope("p_whead"):
            for c in cs:
                pl.when(ctx < nctx - 1)(lambda: head_mr(c).wait_recv())

        @pl.when((ctx < nctx - 1) & (cs[-1] == nblk - 1))
        def _():
            each(nblk, lambda c: tail_mr(c).start())

        found = [dot(fg[...], gfull[c]) for c in cs]
        mixes = []
        for c, gs in zip(cs, found):
            zs[c] = gs
            gr, gi = gs[:half], gs[half:]
            hr, hi = hs[c, :half, :], hs[c, half:, :]
            mixes.append(spectrum_of(gr * hr + gi * hi, gi * hr - gr * hi))
        found = [dot(inv[:rows, :], mix) for mix in mixes]
        for c, gp in zip(cs, found):
            for i in range(cpb):
                cols = slice(i * LANES, (i + 1) * LANES)
                back, value = gp[:, cols], normed[c, :, cols]
                grad = back * km[c, :, cols].astype(F32)
                qm[c, :, cols] = (back * value).astype(BF16)
                normed[c, :, cols] = grad
                acc[:rows, :] += grad * value

    with jax.named_scope("p_adj"):
        several(0, nblk, adjoint_step)
    send_rows(1)

    def corr_step(cs):
        found = [dot(fz[:, taps:], zfull[c, taps:, :]) for c in cs]
        mixes = []
        for c, value in zip(cs, found):
            gr, gi = zs[c, :half, :], zs[c, half:, :]
            zr, zi = value[:half], value[half:]
            mixes.append(spectrum_of(gr * zr + gi * zi, gi * zr - gr * zi))
            zs[c] = value
        found = [dot(inv[:taps, :], mix) for mix in mixes]
        for c, part in zip(cs, found):
            for p in range(ppb):
                corr[c * ppb + p] = part[:, p * group : (p + 1) * group]

    with jax.named_scope("p_corr1"):
        several(0, nblk // 2, corr_step)

    with jax.named_scope("p_weight"):
        weight = as_column(sum_rows(1))
        coef[...] = weight * (scale[...] * scale[...]) * (1.0 / width)

    def edge_step(c):
        for i in range(cpb):
            cols = slice(i * LANES, (i + 1) * LANES)
            at = pl.ds(pl.multiple_of(c * blk + i * LANES, LANES), LANES)
            quer = q[c, :halo, cols].astype(F32)
            mixed = quer * conv[c, :halo, cols]
            back = normed[c, :halo, cols] * scale[:halo, :]
            gm = gain[c, :, cols] * back - mixed * coef[:halo, :]
            head_out[:, at] = (gm * quer).astype(BF16)

    each(nblk, edge_step)
    pl.when(ctx > 0)(head_se.start)

    with jax.named_scope("p_corr2"):
        several(nblk // 2, nblk, corr_step)

    mine = ctx // ratio

    def part_of(s, i, other):
        index = 0
        for n, bit in enumerate(bits):
            size = bit // ratio
            own = lax.rem(mine // size, 2)
            if n < s:
                index = index + own * size
            elif n == s:
                index = index + (1 - own if other else own) * size
            else:
                index = index + lax.rem(i // 2 ** (n - s - 1), 2) * size
        return index

    def span(s):
        count = parts >> (s + 1)
        return parts - 2 * count, count

    def halve_copy(s):
        begin, count = span(s)
        bit = bits[s]
        partner = ctx + bit - 2 * bit * lax.rem(ctx // bit, 2)
        where = pl.ds(begin, count)
        return remote(away.at[where], got.at[where], halve_send.at[s], halve_recv.at[s],
                      {"ctx": partner})

    def halve_start(s):
        begin, count = span(s)

        def body(i):
            away[begin + i] = corr[part_of(s, i, True)].astype(BF16)

        each(count, body)
        halve_copy(s).start()

    def halve_end(s):
        begin, count = span(s)
        halve_copy(s).wait_recv()

        def body(i):
            corr[part_of(s, i, False)] += got[begin + i].astype(F32)

        each(count, body)

    halve_start(0)

    with jax.named_scope("p_headse"):
        pl.when(ctx < nctx - 1)(head_se.wait_recv)

    high = next(n for n in (32, 16, rows) if rows % n == 0)
    lanes = runs(cpb)

    def back_lane(c, i, n):
        cols = pl.ds(pl.multiple_of(i * LANES, LANES), LANES)
        lane = c * cpb + i
        at = pl.ds(pl.multiple_of(lane * LANES, LANES), LANES)
        pad_g[n, rows:, :] = head_in[:, at].astype(F32)
        gains = jnp.zeros((8, LANES), F32)
        sums = [jnp.zeros((8, LANES), F32) for _ in range(taps_se)]

        def fold(value):
            return jnp.sum(value.reshape(-1, 8, LANES), axis=0)

        taps_of = [fse[c, j : j + 1, cols] for j in range(taps_se)]
        gain_of = gain[c, :, cols]
        for start in range(rows - high, -1, -high):
            at_rows = slice(start, start + high)
            back = normed[c, at_rows, cols] * scale[at_rows, :]
            quer = q[c, at_rows, cols].astype(F32)
            value = conv[c, at_rows, cols]
            mixed = quer * value
            gm = gain_of * back - mixed * coef[at_rows, :]
            gains = gains + fold(back * mixed)
            q[c, at_rows, cols] = (gm * value).astype(BF16)
            gc = (gm * quer).astype(BF16).astype(F32)
            pad_g[n, at_rows, :] = gc
            gp = taps_of[0] * gc
            for j in range(taps_se):
                if j:
                    gp = gp + taps_of[j] * pad_g[n, pl.ds(start + j, high), :]
                sums[j] = sums[j] + fold(gc * prod[lane, pl.ds(start + halo - j, high), :])
            key = k[c, at_rows, cols].astype(F32)
            k[c, at_rows, cols] = (gp * v[c, at_rows, cols].astype(F32)).astype(BF16)
            v[c, at_rows, cols] = (gp * key).astype(BF16)
        part = lane * LANES // group
        place = pl.ds(pl.multiple_of(lax.rem(lane * LANES, group), LANES), LANES)
        for j, value in enumerate(sums + [gains]):
            small[part, j : j + 1, place] = jnp.sum(value, axis=0, keepdims=True)

    def back_step(p):
        c, i = (p * lanes) // cpb, lax.rem(p * lanes, cpb)
        for n in range(lanes):
            back_lane(c, i + n, n)

    def swap(step):
        there = lax.rem(ctx + step, nctx)
        return remote(small.at[there], small_in.at[step - 1], swap_send.at[step - 1],
                      swap_recv.at[step - 1], {"ctx": there})

    def medium_step(cs):
        with jax.named_scope("p_wtail"):
            for c in cs:
                pl.when(ctx > 0)(lambda: tail_mr(c).wait_recv())
        found = [dot(fz[:, :taps], zfull[c, :taps, :]) for c in cs]
        mixes = []
        for c, value in zip(cs, found):
            zr, zi = zs[c, :half, :] + value[:half], zs[c, half:, :] + value[half:]
            hr, hi = hs[c, :half, :], hs[c, half:, :]
            mixes.append(spectrum_of(zr * hr - zi * hi, zr * hi + zi * hr))
        found = [dot(inv[:rows, :], mix) for mix in mixes]
        for c, value in zip(cs, found):
            up[c] = (up[c].astype(F32) * value).astype(BF16)

    def pass_on(s):
        with jax.named_scope("p_halve"):
            halve_end(s)
            if s + 1 < steps:
                halve_start(s + 1)

    steps = len(bits)
    per = nblk * cpb // lanes
    early = per // 4
    with jax.named_scope("p_back"):
        each(early, back_step)
    pass_on(0)
    with jax.named_scope("p_back"):
        each(per - early, back_step, early)
    if ratio == 1:
        for step in range(1, nctx):
            swap(step).start()
    pass_on(1)
    with jax.named_scope("p_medium"):
        several(0, nblk, medium_step)
    for s in range(2, steps):
        pass_on(s)

    with jax.named_scope("p_swap"):
        total_o[...] = corr[mine] * factor
        if ratio == 1:
            value = small[mine]
            for step in range(1, nctx):
                swap(step).wait_recv()
                value = value + small_in[step - 1]
            small_o[...] = value * factor
        else:
            small_o[...] = small[...]

    with jax.named_scope("p_fin"):
        @pl.when(ctx > 0)
        def _():
            each(nblk, lambda c: head_mr(c).wait_send())
            head_se.wait_send()

        @pl.when(ctx < nctx - 1)
        def _():
            each(nblk, lambda c: tail_mr(c).wait_send())
            tail_se.wait_send()

        for which in range(2):
            for step in range(1, ntp):
                row_copy(which, step).wait_send()
        for s in range(steps):
            halve_copy(s).wait_send()
        if ratio == 1:
            for step in range(1, nctx):
                swap(step).wait_send()


def output_kernel(whole, *refs):
    count = 9 if whole else 5
    q, k, v, qm, up, total, small = refs[:7]
    outs, (sems,) = refs[7 : 7 + count], refs[7 + count :]
    gq_o, gk_o, gv_o, gqm_o, gkm_o = outs[:5]
    nblk, rows, blk = q.shape

    def copy(src, dst, s, c):
        at = pl.ds(pl.multiple_of(c * blk, blk), blk)
        return pltpu.make_async_copy(src.at[c], dst.at[:, at], sems.at[s, c])

    streams = ((q, gq_o), (k, gk_o), (v, gv_o), (qm, gkm_o), (up, gqm_o))

    def begin(c, carry):
        for s in range(5):
            copy(*streams[s], s, c).start()
        return carry

    lax.fori_loop(0, nblk, begin, 0)
    if whole:
        filter_se, filter_mr, skip, gain = outs[5:]
        taps_se = filter_se.shape[0]
        filter_se[...] = small[:taps_se, :]
        filter_mr[...] = total[...]
        skip[...] = total[0:1, :]
        gain[...] = small[taps_se : taps_se + 1, :]
    def end(c, carry):
        for s in range(5):
            copy(*streams[s], s, c).wait()
        return carry

    lax.fori_loop(0, nblk, end, 0)


def split_parts(parts, share):
    count, height, group = parts.shape
    if group == share:
        return parts
    parts = parts.reshape(count, height, group // share, share)
    return parts.transpose(0, 2, 1, 3).reshape(-1, height, share)


def scatter_sum(parts, axis, stop):
    size = lax.axis_size(axis)
    me = lax.axis_index(axis)
    bit = 1
    while bit < stop:
        rest = parts.reshape((parts.shape[0] // 2, 2) + parts.shape[1:])
        mine = lax.rem(me // bit, 2)
        away = lax.dynamic_index_in_dim(rest, 1 - mine, 1, keepdims=False).astype(BF16)
        keep = lax.dynamic_index_in_dim(rest, mine, 1, keepdims=False)
        with jax.named_scope(f"halve_{bit}"):
            got = lax.ppermute(away, axis, [(i, i ^ bit) for i in range(size)])
        parts = keep + got.astype(F32)
        bit *= 2
    return parts[0]


def local(
    query_se, key_se, value_se, query_mr, key_mr, upstream, filter_se, filter_mr, skip_mr, norm_gain
):
    rows, chans = query_se.shape
    taps_se, taps = filter_se.shape[0], filter_mr.shape[0]
    ctx, ntp = lax.axis_size("ctx"), lax.axis_size("tp")
    width = chans * ntp
    tokens = rows * ctx
    share = chans // ctx
    group = up_to(share, LANES)
    halo = up_to(taps_se - 1, 16)
    blk = max(group, min(512, chans))
    nblk = chans // blk
    fz, fg, inv = transforms(rows, taps)
    length = rows + taps
    tall = up_to(rows, LANES)
    nlane = chans // LANES

    def out(shape, kind):
        return jax.ShapeDtypeStruct(shape, kind)

    ins = (query_se, key_se, value_se, query_mr, key_mr, upstream, filter_se, filter_mr,
           skip_mr[None], norm_gain[None], fg, fz, inv)
    V, D = pltpu.VMEM, pltpu.SemaphoreType.DMA
    ratio = group // share
    parts = chans // group
    small_height = taps_se + 1
    small_shape = (small_height, group) if ratio == 1 else (parts, small_height, group)
    stream = V((nblk, rows, blk), BF16)
    outs = [stream] * 5 + [V((taps, group), F32), V(small_shape, F32)]
    lanes = runs(blk // LANES)
    steps = len(halving_bits(ctx, ratio))
    scratch = [
        stream, V((nblk, taps_se, blk), F32), V((nblk, taps, blk), F32), V((nblk, 1, blk), F32),
        V((nblk, 1, blk), F32), V(fg.shape, BF16), V(fz.shape, BF16), V(inv.shape, BF16),
        V((2, halo, chans), BF16), V((halo, chans), BF16), V((halo, chans), BF16),
        V((halo, chans), BF16), V((halo, chans), BF16),
        V((nblk, length, blk), BF16), V((nblk, length, blk), BF16),
        V((nblk, rows, blk), F32), V((nblk, rows, blk), F32),
        V((nblk, length, blk), F32), V((nblk, length, blk), F32),
        V((nlane, halo + rows, LANES), F32), V((lanes, halo + rows, LANES), F32),
        V((parts, taps, group), F32), V((parts, small_height, group), F32),
        V((parts, taps, group), BF16), V((parts, taps, group), BF16),
        V((max(ctx - 1, 1), small_height, group), F32),
        V((tall, LANES), F32), V((rows, LANES), F32), V((rows, LANES), F32),
        V((2, 8, tall), F32), V((2, max(ntp - 1, 1), 8, tall), F32),
        D((7, nblk)), D((3, nblk)), D((5,)), D((2,)), D((2,)),
        D((nblk,)), D((nblk,)), D((nblk,)), D((nblk,)),
        D((2, max(ntp - 1, 1))), D((2, max(ntp - 1, 1))),
        D((steps,)), D((steps,)), D((max(ctx - 1, 1),)), D((max(ctx - 1, 1),)),
    ]
    anywhere = pl.BlockSpec(memory_space=pl.ANY)
    inside = pl.BlockSpec(memory_space=pltpu.VMEM)
    with jax.named_scope("layer"):
        held = pl.pallas_call(
            functools.partial(layer_kernel, width, tokens, ctx, ntp, ratio),
            name="layer",
            in_specs=[anywhere] * len(ins),
            out_specs=[inside] * len(outs),
            out_shape=outs,
            scratch_shapes=scratch,
            compiler_params=pltpu.CompilerParams(
                collective_id=0, has_side_effects=True, vmem_limit_bytes=48 * 2**20
            ),
        )(*ins)

    def out(shape, kind):
        return jax.ShapeDtypeStruct(shape, kind)

    results = [out((rows, chans), BF16)] * 5
    specs = [anywhere] * 5
    if ratio == 1:
        results += [out((n, share), F32) for n in (taps_se, taps, 1, 1)]
        specs += [inside] * 4
    with jax.named_scope("output"):
        found = pl.pallas_call(
            functools.partial(output_kernel, ratio == 1),
            name="output",
            in_specs=[inside] * len(held),
            out_specs=specs,
            out_shape=results,
            scratch_shapes=[D((5, nblk))],
            compiler_params=pltpu.CompilerParams(vmem_limit_bytes=8 * 2**20),
        )(*[pltpu.with_memory_space_constraint(a, pltpu.VMEM) for a in held])
    if ratio == 1:
        return (*found[:7], found[7].reshape(share), found[8].reshape(share))
    total_mr, small = held[5], held[6]
    total_mr = scatter_sum(split_parts(total_mr[None], share), "ctx", ratio)
    small = lax.all_to_all(split_parts(small, share), "ctx", 0, 0, tiled=True)
    total = jnp.sum(small, axis=0) * (1.0 / math.sqrt(tokens))
    return (*found, total[:taps_se], total_mr, total_mr[0], total[taps_se])


def solution(mesh):
    streams = (P("ctx", "tp"),)
    in_specs = streams * 6 + (P(None, "tp"), P(None, "tp"), P("tp"), P("tp"))
    both = ("tp", "ctx")
    out_specs = streams * 5 + (P(None, both), P(None, both), P(both), P(both))
    return jax.shard_map(local, mesh=mesh, in_specs=in_specs, out_specs=out_specs, check_vma=False)
```

```python
import functools
import math

import jax
import jax.numpy as jnp
import numpy as np
from jax import lax
from jax.experimental import pallas as pl
from jax.experimental.pallas import tpu as pltpu
from jax.sharding import PartitionSpec as P

EPSILON = 0.1
F32 = jnp.float32
BF16 = jnp.bfloat16
LANES = 128
MESH = pl.DeviceIdType.MESH


def transforms(rows, taps):
    length = rows + taps
    freq = 2.0 * np.pi * (np.arange(length // 2) + 0.5) / length

    def forward(start, stop):
        angle = freq[:, None] * np.arange(start, stop)[None, :]
        return np.concatenate([np.cos(angle), -np.sin(angle)], 0)

    angle = np.arange(max(rows, taps))[:, None] * freq[None, :]
    inverse = np.concatenate([np.cos(angle), -np.sin(angle)], 1) * (2.0 / length)
    mats = forward(-taps, rows), forward(0, length), inverse
    return [jnp.asarray(m, BF16) for m in mats]


def dot(a, b):
    return jnp.dot(a, b, preferred_element_type=F32)


def spectrum_of(real, imag):
    return jnp.concatenate([real.astype(BF16), imag.astype(BF16)], 0)


def up_to(value, step):
    return -(-value // step) * step


def halving_bits(size, ratio):
    bits = []
    bit = ratio
    while bit < size:
        bits.append(bit)
        bit *= 2
    return bits[:1] + bits[2:3] + bits[1:2] + bits[3:]


def runs(count):
    return 2 if count % 2 == 0 else 1


def layer_kernel(width, tokens, nctx, ntp, ratio, *refs):
    (q_h, k_h, v_h, qm_h, km_h, up_h, fse_h, fmr_h, skip_h, gain_h, fg_h, fz_h, inv_h,
     q, k, v, qm, up, total_o, small_o,
     km, fse, fmr, skip, gain, fg, fz, inv, ends, tail_out, tail_in, head_out, head_in,
     gfull, zfull, conv, normed, hs, zs, prod, pad_g, lasts, corr, small, away, got, small_in,
     acc, scale, coef, row_out, row_in,
     in_sem, small_sem, edge_sem, edge_send, edge_recv, head_send, head_recv, tail_send, tail_recv,
     row_send, row_recv, halve_send, halve_recv, swap_send, swap_recv) = refs
    nblk, rows, blk = q.shape
    taps_se, taps = fse.shape[1], fmr.shape[1]
    edge, halo = ends.shape[1], prod.shape[1] - rows
    half = fg.shape[0] // 2
    parts, _, group = corr.shape
    ppb = parts // nblk
    cpb = blk // LANES
    ctx, tp = lax.axis_index("ctx"), lax.axis_index("tp")
    first, last = ctx == 0, ctx == nctx - 1
    bits = halving_bits(nctx, ratio)
    factor = 1.0 / math.sqrt(tokens)

    def cols_of(c):
        return pl.ds(pl.multiple_of(c * blk, blk), blk)

    def each(count, body, start=0):
        def step(c, carry):
            body(c)
            return carry
        lax.fori_loop(start, start + count, step, 0)

    def several(start, stop, body):
        n = runs(stop - start)
        each((stop - start) // n, lambda p: body([start + p * n + u for u in range(n)]))

    def remote(src, dst, send, recv, where):
        return pltpu.make_async_remote_copy(
            src_ref=src, dst_ref=dst, send_sem=send, recv_sem=recv,
            device_id=where, device_id_type=MESH,
        )

    streams = ((up_h, up), (qm_h, qm), (k_h, k), (v_h, v), (q_h, q), (km_h, km), (fmr_h, fmr))

    def load(s, c):
        src, dst = streams[s]
        return pltpu.make_async_copy(src.at[:, cols_of(c)], dst.at[c], in_sem.at[s, c])

    def wide(s, c):
        src, dst = ((fse_h, fse), (skip_h, skip), (gain_h, gain))[s]
        return pltpu.make_async_copy(src.at[:, cols_of(c)], dst.at[c], small_sem.at[s, c])

    def single(s):
        bottom = pl.ds(rows - edge, edge)
        src, dst = ((k_h.at[bottom, :], ends.at[0]), (v_h.at[bottom, :], ends.at[1]),
                    (fg_h, fg), (fz_h, fz), (inv_h, inv))[s]
        return pltpu.make_async_copy(src, dst, edge_sem.at[s])

    barrier = pltpu.get_barrier_semaphore()
    for step in range(1, nctx):
        pl.semaphore_signal(barrier, inc=1, device_id={"ctx": lax.rem(ctx + step, nctx)},
                            device_id_type=MESH)
    for step in range(1, ntp):
        pl.semaphore_signal(barrier, inc=1, device_id={"tp": lax.rem(tp + step, ntp)},
                            device_id_type=MESH)

    def start_group(*which):
        def body(c):
            for s in which:
                load(s, c).start()
        each(nblk, body)

    def start_wide(c):
        for s in range(3):
            wide(s, c).start()

    single(0).start()
    single(1).start()
    start_group(0, 1)
    single(3).start()
    each(nblk, start_wide)
    start_group(6)
    start_group(2, 3, 4)
    single(2).start()
    single(4).start()
    start_group(5)

    @pl.when(first)
    def _():
        tail_in[...] = jnp.zeros_like(tail_in)
        zfull[:, :taps, :] = jnp.zeros((nblk, taps, blk), BF16)

    @pl.when(last)
    def _():
        head_in[...] = jnp.zeros_like(head_in)
        gfull[:, rows:, :] = jnp.zeros((nblk, taps, blk), BF16)

    before, after = {"ctx": ctx - 1}, {"ctx": ctx + 1}
    tail_se = remote(tail_out, tail_in, edge_send.at[0], edge_recv.at[0], after)
    head_se = remote(head_out, head_in, edge_send.at[1], edge_recv.at[1], before)

    def head_mr(c):
        return remote(gfull.at[c, pl.ds(0, taps), :], gfull.at[c, pl.ds(rows, taps), :],
                      head_send.at[c], head_recv.at[c], before)

    def tail_mr(c):
        return remote(zfull.at[c, pl.ds(rows, taps), :], zfull.at[c, pl.ds(0, taps), :],
                      tail_send.at[c], tail_recv.at[c], after)

    single(0).wait()
    single(1).wait()
    ending = (ends[0].astype(F32) * ends[1].astype(F32))[edge - halo :]
    middle = nblk // 2
    tail_out[...] = jnp.concatenate(
        [ending[:, : middle * blk], ending[:, middle * blk :]], 0
    ).astype(BF16)

    def received(buffer, c, i):
        at = pl.ds(pl.multiple_of(lax.rem(c, middle) * blk + i * LANES, LANES), LANES)
        both = buffer[:, at].astype(F32)
        return jnp.where(c >= middle, both[halo:], both[:halo])

    def gate_step(c):
        load(0, c).wait()
        load(1, c).wait()
        gfull[c, :rows, :] = (up[c].astype(F32) * qm[c].astype(F32)).astype(BF16)

    with jax.named_scope("p_gate"):
        each(nblk, gate_step)
    with jax.named_scope("p_bar"):
        pl.semaphore_wait(barrier, nctx + ntp - 2)
    pl.when(ctx < nctx - 1)(tail_se.start)
    single(3).wait()

    def filter_step(cs):
        for c in cs:
            load(6, c).wait()
            wide(1, c).wait()
        found = [dot(fz[:, taps : 2 * taps], fmr[c].astype(BF16)) for c in cs]
        for c, value in zip(cs, found):
            hs[c, :half, :] = value[:half] + skip[c]
            hs[c, half:, :] = value[half:]

    with jax.named_scope("p_filt1"):
        several(0, nblk // 4, filter_step)

    @pl.when(ctx > 0)
    def _():
        each(nblk, lambda c: head_mr(c).start())

    acc[...] = jnp.zeros_like(acc)
    prod[:, :halo, :] = jnp.zeros((prod.shape[0], halo, LANES), F32)

    def short_conv(c, cols, lane, height):
        out = fse[c, 0:1, cols] * prod[lane, pl.ds(halo, height), :]
        for j in range(1, taps_se):
            out = out + fse[c, j : j + 1, cols] * prod[lane, pl.ds(halo - j, height), :]
        conv[c, :height, cols] = out
        mixed = q[c, :height, cols].astype(F32) * out
        return mixed * mixed

    def short_step(c):
        wide(0, c).wait()
        wide(2, c).wait()
        for s in range(3):
            load(2 + s, c).wait()
        for i in range(cpb):
            cols = slice(i * LANES, (i + 1) * LANES)
            lane = c * cpb + i
            product = k[c, :, cols].astype(F32) * v[c, :, cols].astype(F32)
            prod[lane, halo:, :] = product.astype(BF16).astype(F32)
            acc[halo:rows, :] += short_conv(c, cols, lane, rows)[halo:]

    def top_step(c):
        for i in range(cpb):
            cols = slice(i * LANES, (i + 1) * LANES)
            lane = c * cpb + i
            prod[lane, :halo, :] = received(tail_in, c, i)
            acc[:halo, :] += short_conv(c, cols, lane, halo)

    with jax.named_scope("p_short"):
        each(nblk, short_step)
    with jax.named_scope("p_tailse"):
        pl.when(ctx > 0)(tail_se.wait_recv)
    with jax.named_scope("p_top"):
        each(nblk, top_step)

    def row_copy(which, step):
        return remote(row_out.at[which], row_in.at[which, step - 1],
                      row_send.at[which, step - 1], row_recv.at[which, step - 1],
                      {"tp": lax.rem(tp + step, ntp)})

    def send_rows(which):
        total = jnp.sum(jnp.transpose(acc[...]), axis=0, keepdims=True)
        row_out[which] = jnp.broadcast_to(total, row_out.shape[1:])
        for step in range(1, ntp):
            row_copy(which, step).start()

    def sum_rows(which):
        total = row_out[which]
        for step in range(1, ntp):
            row_copy(which, step).wait_recv()
            total = total + row_in[which, step - 1]
        return total[0:1, :]

    def as_column(line):
        return jnp.transpose(jnp.broadcast_to(line, (LANES, line.shape[1])))[:rows, :]

    send_rows(0)
    with jax.named_scope("p_filt2"):
        several(nblk // 4, nblk, filter_step)
    acc[...] = jnp.zeros_like(acc)
    with jax.named_scope("p_scale"):
        scale[...] = as_column(lax.rsqrt(sum_rows(0) * (1.0 / width) + EPSILON))

    def product_step(c):
        load(5, c).wait()
        for i in range(cpb):
            cols = slice(i * LANES, (i + 1) * LANES)
            mixed = q[c, :, cols].astype(F32) * conv[c, :, cols]
            value = mixed * scale[...] * gain[c, :, cols]
            normed[c, :, cols] = value
            zfull[c, taps:, cols] = (km[c, :, cols].astype(F32) * value).astype(BF16)

    with jax.named_scope("p_prod"):
        each(nblk, product_step)

    single(2).wait()
    single(4).wait()

    def tails(start, stop):
        pl.when(ctx < nctx - 1)(lambda: each(stop - start, lambda c: tail_mr(c).start(), start))

    ahead = nblk * 3 // 8
    late = lax.rem(ctx, 4) == 3

    def adjoint_step(cs):
        with jax.named_scope("p_whead"):
            for c in cs:
                pl.when(ctx < nctx - 1)(lambda: head_mr(c).wait_recv())

        @pl.when(cs[-1] == nblk - 1)
        def _():
            tails(0, ahead)
            pl.when(jnp.logical_not(late))(lambda: tails(ahead, nblk))

        gss = [dot(fg[...], gfull[c]) for c in cs]
        zss = [dot(fz[:, taps:], zfull[c, taps:, :]) for c in cs]
        mixes, pairs = [], []
        for c, gs, value in zip(cs, gss, zss):
            gr, gi = gs[:half], gs[half:]
            hr, hi = hs[c, :half, :], hs[c, half:, :]
            mixes.append(spectrum_of(gr * hr + gi * hi, gi * hr - gr * hi))
            zr, zi = value[:half], value[half:]
            pairs.append(spectrum_of(gr * zr + gi * zi, gi * zr - gr * zi))
            zs[c] = value
        found = [dot(inv[:rows, :], mix) for mix in mixes]
        parts_of = [dot(inv[:taps, :], mix) for mix in pairs]
        for c, gp, part in zip(cs, found, parts_of):
            for i in range(cpb):
                cols = slice(i * LANES, (i + 1) * LANES)
                back, value = gp[:, cols], normed[c, :, cols]
                grad = back * km[c, :, cols].astype(F32)
                qm[c, :, cols] = (back * value).astype(BF16)
                normed[c, :, cols] = grad
                acc[:rows, :] += grad * value
            for p in range(ppb):
                corr[c * ppb + p] = part[:, p * group : (p + 1) * group]

    with jax.named_scope("p_adj"):
        several(0, nblk, adjoint_step)
    send_rows(1)
    mine = ctx // ratio

    def part_of(s, i, other):
        index = 0
        for n, bit in enumerate(bits):
            size = bit // ratio
            own = lax.rem(mine // size, 2)
            if n < s:
                index = index + own * size
            elif n == s:
                index = index + (1 - own if other else own) * size
            else:
                index = index + lax.rem(i // 2 ** (n - s - 1), 2) * size
        return index

    def span(s):
        count = parts >> (s + 1)
        return parts - 2 * count, count

    def halve_copy(s):
        begin, count = span(s)
        bit = bits[s]
        partner = ctx + bit - 2 * bit * lax.rem(ctx // bit, 2)
        where = pl.ds(begin, count)
        return remote(away.at[where], got.at[where], halve_send.at[s], halve_recv.at[s],
                      {"ctx": partner})

    def halve_start(s):
        begin, count = span(s)

        def body(i):
            away[begin + i] = corr[part_of(s, i, True)].astype(BF16)

        each(count, body)
        halve_copy(s).start()

    def halve_end(s):
        begin, count = span(s)
        halve_copy(s).wait_recv()

        def body(i):
            corr[part_of(s, i, False)] += got[begin + i].astype(F32)

        each(count, body)

    steps = len(bits)

    def pass_on(s):
        with jax.named_scope("p_halve"):
            halve_end(s)
            if s + 1 < steps:
                halve_start(s + 1)

    halve_start(0)
    pass_on(0)
    pl.when(late)(lambda: tails(ahead, nblk))

    with jax.named_scope("p_weight"):
        weight = as_column(sum_rows(1))
        coef[...] = weight * (scale[...] * scale[...]) * (1.0 / width)

    def edge_step(c):
        for i in range(cpb):
            cols = slice(i * LANES, (i + 1) * LANES)
            at = pl.ds(pl.multiple_of(c * blk + i * LANES, LANES), LANES)
            both = []
            for part in (c, c + middle):
                quer = q[part, :halo, cols].astype(F32)
                mixed = quer * conv[part, :halo, cols]
                back = normed[part, :halo, cols] * scale[:halo, :]
                gm = gain[part, :, cols] * back - mixed * coef[:halo, :]
                both.append(gm * quer)
            head_out[:, at] = jnp.concatenate(both, 0).astype(BF16)

    each(middle, edge_step)
    pl.when(ctx > 0)(head_se.start)

    high = next(n for n in (32, 16, rows) if rows % n == 0)
    lanes = runs(cpb)

    def back_lane(c, i, n):
        cols = pl.ds(pl.multiple_of(i * LANES, LANES), LANES)
        lane = c * cpb + i
        pad_g[n, rows:, :] = jnp.zeros((halo, LANES), F32)
        gains = jnp.zeros((8, LANES), F32)
        sums = [jnp.zeros((8, LANES), F32) for _ in range(taps_se)]

        def fold(value):
            return jnp.sum(value.reshape(-1, 8, LANES), axis=0)

        taps_of = [fse[c, j : j + 1, cols] for j in range(taps_se)]
        gain_of = gain[c, :, cols]
        for start in range(rows - high, -1, -high):
            at_rows = slice(start, start + high)
            back = normed[c, at_rows, cols] * scale[at_rows, :]
            quer = q[c, at_rows, cols].astype(F32)
            value = conv[c, at_rows, cols]
            mixed = quer * value
            gm = gain_of * back - mixed * coef[at_rows, :]
            gains = gains + fold(back * mixed)
            q[c, at_rows, cols] = (gm * value).astype(BF16)
            gc = (gm * quer).astype(BF16).astype(F32)
            pad_g[n, at_rows, :] = gc
            if start + high == rows:
                lasts[lane, :halo, :] = gc[high - halo :, :]
            gp = taps_of[0] * gc
            for j in range(taps_se):
                if j:
                    gp = gp + taps_of[j] * pad_g[n, pl.ds(start + j, high), :]
                sums[j] = sums[j] + fold(gc * prod[lane, pl.ds(start + halo - j, high), :])
            key = k[c, at_rows, cols].astype(F32)
            k[c, at_rows, cols] = (gp * v[c, at_rows, cols].astype(F32)).astype(BF16)
            v[c, at_rows, cols] = (gp * key).astype(BF16)
        part = lane * LANES // group
        place = pl.ds(pl.multiple_of(lax.rem(lane * LANES, group), LANES), LANES)
        for j, value in enumerate(sums + [gains]):
            small[part, j : j + 1, place] = jnp.sum(value, axis=0, keepdims=True)

    def bottom_step(c):
        for i in range(cpb):
            cols = slice(i * LANES, (i + 1) * LANES)
            lane = c * cpb + i
            at = pl.ds(pl.multiple_of(lane * LANES, LANES), LANES)
            lasts[lane, halo:, :] = received(head_in, c, i)
            gp = fse[c, 0:1, cols] * lasts[lane, :halo, :]
            for j in range(1, taps_se):
                gp = gp + fse[c, j : j + 1, cols] * lasts[lane, pl.ds(j, halo), :]
            for kept, other in ((k, ends[1, :, at]), (v, ends[0, :, at])):
                old = kept[c, rows - edge :, cols].astype(F32)
                new = gp * other.astype(F32)[edge - halo :]
                kept[c, rows - edge :, cols] = jnp.concatenate(
                    [old[: edge - halo], new], 0
                ).astype(BF16)

    def back_step(p):
        c, i = (p * lanes) // cpb, lax.rem(p * lanes, cpb)
        for n in range(lanes):
            back_lane(c, i + n, n)

    def swap(step):
        there = lax.rem(ctx + step, nctx)
        return remote(small.at[there], small_in.at[step - 1], swap_send.at[step - 1],
                      swap_recv.at[step - 1], {"ctx": there})

    def medium_step(cs):
        with jax.named_scope("p_wtail"):
            for c in cs:
                pl.when(ctx > 0)(lambda: tail_mr(c).wait_recv())
        found = [dot(fz[:, :taps], zfull[c, :taps, :]) for c in cs]
        mixes = []
        for c, value in zip(cs, found):
            zr, zi = zs[c, :half, :] + value[:half], zs[c, half:, :] + value[half:]
            hr, hi = hs[c, :half, :], hs[c, half:, :]
            mixes.append(spectrum_of(zr * hr - zi * hi, zr * hi + zi * hr))
        found = [dot(inv[:rows, :], mix) for mix in mixes]
        for c, value in zip(cs, found):
            up[c] = (up[c].astype(F32) * value).astype(BF16)

    per = nblk * cpb // lanes
    early = per // 2
    with jax.named_scope("p_back"):
        each(early, back_step)
    pass_on(1)
    with jax.named_scope("p_back"):
        each(per - early, back_step, early)
    if ratio == 1:
        for step in range(1, nctx):
            swap(step).start()
    with jax.named_scope("p_headse"):
        pl.when(ctx < nctx - 1)(head_se.wait_recv)
    with jax.named_scope("p_bottom"):
        each(nblk, bottom_step)
    with jax.named_scope("p_medium"):
        several(0, nblk, medium_step)
    for s in range(2, steps):
        pass_on(s)

    with jax.named_scope("p_swap"):
        total_o[...] = corr[mine] * factor
        if ratio == 1:
            value = small[mine]
            for step in range(1, nctx):
                swap(step).wait_recv()
                value = value + small_in[step - 1]
            small_o[...] = value * factor
        else:
            small_o[...] = small[...]

    with jax.named_scope("p_fin"):
        @pl.when(ctx > 0)
        def _():
            each(nblk, lambda c: head_mr(c).wait_send())
            head_se.wait_send()

        @pl.when(ctx < nctx - 1)
        def _():
            each(nblk, lambda c: tail_mr(c).wait_send())
            tail_se.wait_send()

        for which in range(2):
            for step in range(1, ntp):
                row_copy(which, step).wait_send()
        for s in range(steps):
            halve_copy(s).wait_send()
        if ratio == 1:
            for step in range(1, nctx):
                swap(step).wait_send()


def output_kernel(whole, *refs):
    count = 9 if whole else 5
    q, k, v, qm, up, total, small = refs[:7]
    outs, (sems,) = refs[7 : 7 + count], refs[7 + count :]
    gq_o, gk_o, gv_o, gqm_o, gkm_o = outs[:5]
    nblk, rows, blk = q.shape

    def copy(src, dst, s, c):
        at = pl.ds(pl.multiple_of(c * blk, blk), blk)
        return pltpu.make_async_copy(src.at[c], dst.at[:, at], sems.at[s, c])

    streams = ((q, gq_o), (k, gk_o), (v, gv_o), (qm, gkm_o), (up, gqm_o))

    def begin(c, carry):
        for s in range(5):
            copy(*streams[s], s, c).start()
        return carry

    lax.fori_loop(0, nblk, begin, 0)
    if whole:
        filter_se, filter_mr, skip, gain = outs[5:]
        taps_se = filter_se.shape[0]
        filter_se[...] = small[:taps_se, :]
        filter_mr[...] = total[...]
        skip[...] = total[0:1, :]
        gain[...] = small[taps_se : taps_se + 1, :]

    def end(c, carry):
        for s in range(5):
            copy(*streams[s], s, c).wait()
        return carry

    lax.fori_loop(0, nblk, end, 0)


def split_parts(parts, share):
    count, height, group = parts.shape
    if group == share:
        return parts
    parts = parts.reshape(count, height, group // share, share)
    return parts.transpose(0, 2, 1, 3).reshape(-1, height, share)


def scatter_sum(parts, axis, stop):
    size = lax.axis_size(axis)
    me = lax.axis_index(axis)
    bit = 1
    while bit < stop:
        rest = parts.reshape((parts.shape[0] // 2, 2) + parts.shape[1:])
        mine = lax.rem(me // bit, 2)
        away = lax.dynamic_index_in_dim(rest, 1 - mine, 1, keepdims=False).astype(BF16)
        keep = lax.dynamic_index_in_dim(rest, mine, 1, keepdims=False)
        with jax.named_scope(f"halve_{bit}"):
            got = lax.ppermute(away, axis, [(i, i ^ bit) for i in range(size)])
        parts = keep + got.astype(F32)
        bit *= 2
    return parts[0]


def local(
    query_se, key_se, value_se, query_mr, key_mr, upstream, filter_se, filter_mr, skip_mr, norm_gain
):
    rows, chans = query_se.shape
    taps_se, taps = filter_se.shape[0], filter_mr.shape[0]
    ctx, ntp = lax.axis_size("ctx"), lax.axis_size("tp")
    width = chans * ntp
    tokens = rows * ctx
    share = chans // ctx
    group = up_to(share, LANES)
    halo, edge = up_to(taps_se - 1, 8), up_to(taps_se - 1, 16)
    blk = max(group, min(512, chans // 2))
    nblk = chans // blk
    fz, fg, inv = transforms(rows, taps)
    length = rows + taps
    tall = up_to(rows, LANES)
    nlane = chans // LANES

    def out(shape, kind):
        return jax.ShapeDtypeStruct(shape, kind)

    ins = (query_se, key_se, value_se, query_mr, key_mr, upstream, filter_se, filter_mr,
           skip_mr[None], norm_gain[None], fg, fz, inv)
    V, D = pltpu.VMEM, pltpu.SemaphoreType.DMA
    ratio = group // share
    parts = chans // group
    small_height = taps_se + 1
    small_shape = (small_height, group) if ratio == 1 else (parts, small_height, group)
    stream = V((nblk, rows, blk), BF16)
    outs = [stream] * 5 + [V((taps, group), F32), V(small_shape, F32)]
    lanes = runs(blk // LANES)
    message = (2 * halo, chans // 2)
    steps = len(halving_bits(ctx, ratio))
    scratch = [
        stream, V((nblk, taps_se, blk), F32), V((nblk, taps, blk), F32), V((nblk, 1, blk), F32),
        V((nblk, 1, blk), F32), V(fg.shape, BF16), V(fz.shape, BF16), V(inv.shape, BF16),
        V((2, edge, chans), BF16), V(message, BF16), V(message, BF16), V(message, BF16),
        V(message, BF16),
        V((nblk, length, blk), BF16), V((nblk, length, blk), BF16),
        V((nblk, rows, blk), F32), V((nblk, rows, blk), F32),
        V((nblk, length, blk), F32), V((nblk, length, blk), F32),
        V((nlane, halo + rows, LANES), F32), V((lanes, halo + rows, LANES), F32),
        V((nlane, 2 * halo, LANES), F32),
        V((parts, taps, group), F32), V((parts, small_height, group), F32),
        V((parts, taps, group), BF16), V((parts, taps, group), BF16),
        V((max(ctx - 1, 1), small_height, group), F32),
        V((tall, LANES), F32), V((rows, LANES), F32), V((rows, LANES), F32),
        V((2, 8, tall), F32), V((2, max(ntp - 1, 1), 8, tall), F32),
        D((7, nblk)), D((3, nblk)), D((5,)), D((2,)), D((2,)),
        D((nblk,)), D((nblk,)), D((nblk,)), D((nblk,)),
        D((2, max(ntp - 1, 1))), D((2, max(ntp - 1, 1))),
        D((steps,)), D((steps,)), D((max(ctx - 1, 1),)), D((max(ctx - 1, 1),)),
    ]
    anywhere = pl.BlockSpec(memory_space=pl.ANY)
    inside = pl.BlockSpec(memory_space=pltpu.VMEM)
    with jax.named_scope("layer"):
        held = pl.pallas_call(
            functools.partial(layer_kernel, width, tokens, ctx, ntp, ratio),
            name="layer",
            in_specs=[anywhere] * len(ins),
            out_specs=[inside] * len(outs),
            out_shape=outs,
            scratch_shapes=scratch,
            compiler_params=pltpu.CompilerParams(
                collective_id=0, has_side_effects=True, vmem_limit_bytes=48 * 2**20
            ),
        )(*ins)

    def out(shape, kind):
        return jax.ShapeDtypeStruct(shape, kind)

    results = [out((rows, chans), BF16)] * 5
    specs = [anywhere] * 5
    if ratio == 1:
        results += [out((n, share), F32) for n in (taps_se, taps, 1, 1)]
        specs += [inside] * 4
    with jax.named_scope("output"):
        found = pl.pallas_call(
            functools.partial(output_kernel, ratio == 1),
            name="output",
            in_specs=[inside] * len(held),
            out_specs=specs,
            out_shape=results,
            scratch_shapes=[D((5, nblk))],
            compiler_params=pltpu.CompilerParams(vmem_limit_bytes=8 * 2**20),
        )(*[pltpu.with_memory_space_constraint(a, pltpu.VMEM) for a in held])
    if ratio == 1:
        return (*found[:7], found[7].reshape(share), found[8].reshape(share))
    total_mr, small = held[5], held[6]
    total_mr = scatter_sum(split_parts(total_mr[None], share), "ctx", ratio)
    small = lax.all_to_all(split_parts(small, share), "ctx", 0, 0, tiled=True)
    total = jnp.sum(small, axis=0) * (1.0 / math.sqrt(tokens))
    return (*found, total[:taps_se], total_mr, total_mr[0], total[taps_se])


def solution(mesh):
    streams = (P("ctx", "tp"),)
    in_specs = streams * 6 + (P(None, "tp"), P(None, "tp"), P("tp"), P("tp"))
    both = ("tp", "ctx")
    out_specs = streams * 5 + (P(None, both), P(None, both), P(both), P(both))
    return jax.shard_map(local, mesh=mesh, in_specs=in_specs, out_specs=out_specs, check_vma=False)
```

```python
import functools
import math

import jax
import jax.numpy as jnp
import numpy as np
from jax import lax
from jax.experimental import pallas as pl
from jax.experimental.pallas import tpu as pltpu
from jax.sharding import PartitionSpec as P

EPSILON = 0.1
F32 = jnp.float32
BF16 = jnp.bfloat16
LANES = 128
MESH = pl.DeviceIdType.MESH


def transforms(rows, taps):
    length = rows + taps
    freq = 2.0 * np.pi * (np.arange(length // 2) + 0.5) / length

    def forward(start, stop):
        angle = freq[:, None] * np.arange(start, stop)[None, :]
        return np.concatenate([np.cos(angle), -np.sin(angle)], 0)

    angle = np.arange(max(rows, taps))[:, None] * freq[None, :]
    inverse = np.concatenate([np.cos(angle), -np.sin(angle)], 1) * (2.0 / length)
    mats = forward(-taps, rows), forward(0, length), inverse
    return [jnp.asarray(m, BF16) for m in mats]


def dot(a, b):
    return jnp.dot(a, b, preferred_element_type=F32)


def spectrum_of(real, imag):
    return jnp.concatenate([real.astype(BF16), imag.astype(BF16)], 0)


def up_to(value, step):
    return -(-value // step) * step


def halving_bits(size, ratio):
    bits = []
    bit = ratio
    while bit < size:
        bits.append(bit)
        bit *= 2
    return bits[:1] + bits[2:] + bits[1:2]


def runs(count):
    return 2 if count % 2 == 0 else 1


def layer_kernel(width, tokens, nctx, ntp, ratio, *refs):
    (q_h, k_h, v_h, qm_h, km_h, up_h, fse_h, fmr_h, skip_h, gain_h, fg_h, fz_h, inv_h,
     q, k, v, qm, up, total_o, small_o,
     km, fse, fmr, skip, gain, fg, fz, inv, ends, tail_out, tail_in, head_out, head_in,
     gfull, zfull, conv, normed, hs, zs, prod, pad_g, lasts, corr, small, away, got, small_in,
     acc, scale, coef, row_out, row_in,
     in_sem, small_sem, edge_sem, edge_send, edge_recv, head_send, head_recv, tail_send, tail_recv,
     row_send, row_recv, halve_send, halve_recv, swap_send, swap_recv) = refs
    nblk, rows, blk = q.shape
    batch = runs(nblk)
    taps_se, taps = fse.shape[1], fmr.shape[1]
    edge, halo = ends.shape[1], prod.shape[1] - rows
    half = fg.shape[0] // 2
    parts, _, group = corr.shape
    ppb = parts // nblk
    cpb = blk // LANES
    ctx, tp = lax.axis_index("ctx"), lax.axis_index("tp")
    first, last = ctx == 0, ctx == nctx - 1
    bits = halving_bits(nctx, ratio)
    factor = 1.0 / math.sqrt(tokens)

    def cols_of(c):
        return pl.ds(pl.multiple_of(c * blk, blk), blk)

    def each(count, body, start=0):
        def step(c, carry):
            body(c)
            return carry
        lax.fori_loop(start, start + count, step, 0)

    def several(start, stop, body):
        n = runs(stop - start)
        each((stop - start) // n, lambda p: body([start + p * n + u for u in range(n)]))

    def remote(src, dst, send, recv, where):
        return pltpu.make_async_remote_copy(
            src_ref=src, dst_ref=dst, send_sem=send, recv_sem=recv,
            device_id=where, device_id_type=MESH,
        )

    streams = ((up_h, up), (qm_h, qm), (k_h, k), (v_h, v), (q_h, q), (km_h, km), (fmr_h, fmr))

    def load(s, c):
        src, dst = streams[s]
        return pltpu.make_async_copy(src.at[:, cols_of(c)], dst.at[c], in_sem.at[s])

    def wide(s, c):
        src, dst = ((fse_h, fse), (skip_h, skip), (gain_h, gain))[s]
        return pltpu.make_async_copy(src.at[:, cols_of(c)], dst.at[c], small_sem.at[s])

    def settle(ref, sem):
        pltpu.make_async_copy(ref, ref, sem).wait()

    def single(s):
        bottom = pl.ds(rows - edge, edge)
        src, dst = ((k_h.at[bottom, :], ends.at[0]), (v_h.at[bottom, :], ends.at[1]),
                    (fg_h, fg), (fz_h, fz), (inv_h, inv))[s]
        return pltpu.make_async_copy(src, dst, edge_sem.at[s])

    barrier = pltpu.get_barrier_semaphore()
    for step in range(1, nctx):
        pl.semaphore_signal(barrier, inc=1, device_id={"ctx": lax.rem(ctx + step, nctx)},
                            device_id_type=MESH)
    for step in range(1, ntp):
        pl.semaphore_signal(barrier, inc=1, device_id={"tp": lax.rem(tp + step, ntp)},
                            device_id_type=MESH)

    def start_group(*which):
        def body(c):
            for s in which:
                load(s, c).start()
        each(nblk, body)

    def start_wide(c):
        for s in range(3):
            wide(s, c).start()

    single(0).start()
    single(1).start()
    start_group(0, 1)
    single(3).start()
    start_group(6)
    each(nblk, start_wide)
    start_group(2, 3, 4)
    single(2).start()
    single(4).start()
    start_group(5)

    @pl.when(first)
    def _():
        tail_in[...] = jnp.zeros_like(tail_in)
        zfull[:, :taps, :] = jnp.zeros((nblk, taps, blk), BF16)

    @pl.when(last)
    def _():
        head_in[...] = jnp.zeros_like(head_in)
        gfull[:, rows:, :] = jnp.zeros((nblk, taps, blk), BF16)

    before, after = {"ctx": ctx - 1}, {"ctx": ctx + 1}
    tail_se = remote(tail_out, tail_in, edge_send.at[0], edge_recv.at[0], after)
    head_se = remote(head_out, head_in, edge_send.at[1], edge_recv.at[1], before)

    def head_mr(c):
        return remote(gfull.at[c, pl.ds(0, taps), :], gfull.at[c, pl.ds(rows, taps), :],
                      head_send.at[0], head_recv.at[c // batch], before)

    def tail_mr(c):
        return remote(zfull.at[c, pl.ds(rows, taps), :], zfull.at[c, pl.ds(0, taps), :],
                      tail_send.at[0], tail_recv.at[c // batch], after)

    single(0).wait()
    single(1).wait()
    ending = (ends[0].astype(F32) * ends[1].astype(F32))[edge - halo :]
    middle = nblk // 2
    tail_out[...] = jnp.concatenate(
        [ending[:, : middle * blk], ending[:, middle * blk :]], 0
    ).astype(BF16)

    def received(buffer, c, i):
        at = pl.ds(pl.multiple_of(lax.rem(c, middle) * blk + i * LANES, LANES), LANES)
        both = buffer[:, at].astype(F32)
        return jnp.where(c >= middle, both[halo:], both[:halo])

    settle(up, in_sem.at[0])
    settle(qm, in_sem.at[1])

    def gate_step(c):
        gfull[c, :rows, :] = (up[c].astype(F32) * qm[c].astype(F32)).astype(BF16)

    with jax.named_scope("p_gate"):
        each(nblk, gate_step)
    with jax.named_scope("p_bar"):
        pl.semaphore_wait(barrier, nctx + ntp - 2)
    pl.when(ctx < nctx - 1)(tail_se.start)
    single(3).wait()
    settle(fmr, in_sem.at[6])
    settle(skip, small_sem.at[1])

    def filter_step(cs):
        found = [dot(fz[:, taps : 2 * taps], fmr[c].astype(BF16)) for c in cs]
        for c, value in zip(cs, found):
            hs[c, :half, :] = value[:half] + skip[c]
            hs[c, half:, :] = value[half:]

    with jax.named_scope("p_filt1"):
        several(0, nblk // 4, filter_step)

    @pl.when(ctx > 0)
    def _():
        each(nblk, lambda c: head_mr(c).start())

    acc[...] = jnp.zeros_like(acc)
    prod[:, :halo, :] = jnp.zeros((prod.shape[0], halo, LANES), F32)

    def short_conv(c, cols, lane, height):
        out = fse[c, 0:1, cols] * prod[lane, pl.ds(halo, height), :]
        for j in range(1, taps_se):
            out = out + fse[c, j : j + 1, cols] * prod[lane, pl.ds(halo - j, height), :]
        conv[c, :height, cols] = out
        mixed = q[c, :height, cols].astype(F32) * out
        return mixed * mixed

    settle(fse, small_sem.at[0])
    settle(gain, small_sem.at[2])
    for s, ref in ((2, k), (3, v), (4, q)):
        settle(ref, in_sem.at[s])

    def short_step(c):
        for i in range(cpb):
            cols = slice(i * LANES, (i + 1) * LANES)
            lane = c * cpb + i
            product = k[c, :, cols].astype(F32) * v[c, :, cols].astype(F32)
            prod[lane, halo:, :] = product.astype(BF16).astype(F32)
            acc[halo:rows, :] += short_conv(c, cols, lane, rows)[halo:]

    def top_step(c):
        for i in range(cpb):
            cols = slice(i * LANES, (i + 1) * LANES)
            lane = c * cpb + i
            prod[lane, :halo, :] = received(tail_in, c, i)
            acc[:halo, :] += short_conv(c, cols, lane, halo)

    with jax.named_scope("p_short"):
        each(nblk, short_step)
    with jax.named_scope("p_tailse"):
        pl.when(ctx > 0)(tail_se.wait_recv)
    with jax.named_scope("p_top"):
        each(nblk, top_step)

    def row_copy(which, step):
        return remote(row_out.at[which], row_in.at[which, step - 1],
                      row_send.at[which, step - 1], row_recv.at[which, step - 1],
                      {"tp": lax.rem(tp + step, ntp)})

    def send_rows(which):
        total = jnp.sum(jnp.transpose(acc[...]), axis=0, keepdims=True)
        row_out[which] = jnp.broadcast_to(total, row_out.shape[1:])
        for step in range(1, ntp):
            row_copy(which, step).start()

    def sum_rows(which):
        total = row_out[which]
        for step in range(1, ntp):
            row_copy(which, step).wait_recv()
            total = total + row_in[which, step - 1]
        return total[0:1, :]

    def as_column(line):
        return jnp.transpose(jnp.broadcast_to(line, (LANES, line.shape[1])))[:rows, :]

    send_rows(0)
    with jax.named_scope("p_filt2"):
        several(nblk // 4, nblk, filter_step)
    acc[...] = jnp.zeros_like(acc)
    with jax.named_scope("p_scale"):
        scale[...] = as_column(lax.rsqrt(sum_rows(0) * (1.0 / width) + EPSILON))

    settle(km, in_sem.at[5])

    def product_step(c):
        for i in range(cpb):
            cols = slice(i * LANES, (i + 1) * LANES)
            mixed = q[c, :, cols].astype(F32) * conv[c, :, cols]
            value = mixed * scale[...] * gain[c, :, cols]
            normed[c, :, cols] = value
            zfull[c, taps:, cols] = (km[c, :, cols].astype(F32) * value).astype(BF16)

    with jax.named_scope("p_prod"):
        each(nblk, product_step)

    single(2).wait()
    single(4).wait()

    def tails(start, stop):
        pl.when(ctx < nctx - 1)(lambda: each(stop - start, lambda c: tail_mr(c).start(), start))

    ahead = nblk * 3 // 8
    late = lax.rem(ctx, 4) == 3

    def adjoint_step(cs):
        with jax.named_scope("p_whead"):
            part = gfull.at[pl.ds(cs[0], batch), pl.ds(rows, taps), :]
            pl.when(ctx < nctx - 1)(lambda: settle(part, head_recv.at[cs[0] // batch]))

        @pl.when(cs[-1] == nblk - 1)
        def _():
            tails(0, ahead)
            pl.when(jnp.logical_not(late))(lambda: tails(ahead, nblk))

        gss = [dot(fg[...], gfull[c]) for c in cs]
        zss = [dot(fz[:, taps:], zfull[c, taps:, :]) for c in cs]
        mixes, pairs = [], []
        for c, gs, value in zip(cs, gss, zss):
            gr, gi = gs[:half], gs[half:]
            hr, hi = hs[c, :half, :], hs[c, half:, :]
            mixes.append(spectrum_of(gr * hr + gi * hi, gi * hr - gr * hi))
            zr, zi = value[:half], value[half:]
            pairs.append(spectrum_of(gr * zr + gi * zi, gi * zr - gr * zi))
            zs[c] = value
        found = [dot(inv[:rows, :], mix) for mix in mixes]
        parts_of = [dot(inv[:taps, :], mix) for mix in pairs]
        for c, gp, part in zip(cs, found, parts_of):
            for i in range(cpb):
                cols = slice(i * LANES, (i + 1) * LANES)
                back, value = gp[:, cols], normed[c, :, cols]
                grad = back * km[c, :, cols].astype(F32)
                qm[c, :, cols] = (back * value).astype(BF16)
                normed[c, :, cols] = grad
                acc[:rows, :] += grad * value
            for p in range(ppb):
                corr[c * ppb + p] = part[:, p * group : (p + 1) * group]

    with jax.named_scope("p_adj"):
        several(0, nblk, adjoint_step)
    send_rows(1)
    mine = ctx // ratio

    def part_of(s, i, other):
        index = 0
        for n, bit in enumerate(bits):
            size = bit // ratio
            own = lax.rem(mine // size, 2)
            if n < s:
                index = index + own * size
            elif n == s:
                index = index + (1 - own if other else own) * size
            else:
                index = index + lax.rem(i // 2 ** (n - s - 1), 2) * size
        return index

    def span(s):
        count = parts >> (s + 1)
        return parts - 2 * count, count

    def halve_copy(s):
        begin, count = span(s)
        bit = bits[s]
        partner = ctx + bit - 2 * bit * lax.rem(ctx // bit, 2)
        where = pl.ds(begin, count)
        return remote(away.at[where], got.at[where], halve_send.at[s], halve_recv.at[s],
                      {"ctx": partner})

    def halve_start(s):
        begin, count = span(s)

        def body(i):
            away[begin + i] = corr[part_of(s, i, True)].astype(BF16)

        each(count, body)
        halve_copy(s).start()

    def halve_end(s):
        begin, count = span(s)
        halve_copy(s).wait_recv()

        def body(i):
            corr[part_of(s, i, False)] += got[begin + i].astype(F32)

        each(count, body)

    steps = len(bits)

    def pass_on(s):
        with jax.named_scope("p_halve"):
            halve_end(s)
            if s + 1 < steps:
                halve_start(s + 1)

    halve_start(0)
    pass_on(0)
    pl.when(late)(lambda: tails(ahead, nblk))

    with jax.named_scope("p_weight"):
        weight = as_column(sum_rows(1))
        coef[...] = weight * (scale[...] * scale[...]) * (1.0 / width)

    def edge_step(c):
        for i in range(cpb):
            cols = slice(i * LANES, (i + 1) * LANES)
            at = pl.ds(pl.multiple_of(c * blk + i * LANES, LANES), LANES)
            both = []
            for part in (c, c + middle):
                quer = q[part, :halo, cols].astype(F32)
                mixed = quer * conv[part, :halo, cols]
                back = normed[part, :halo, cols] * scale[:halo, :]
                gm = gain[part, :, cols] * back - mixed * coef[:halo, :]
                both.append(gm * quer)
            head_out[:, at] = jnp.concatenate(both, 0).astype(BF16)

    each(middle, edge_step)
    pl.when(ctx > 0)(head_se.start)

    high = next(n for n in (32, 16, rows) if rows % n == 0)
    lanes = runs(cpb)

    def back_lane(c, i, n):
        cols = pl.ds(pl.multiple_of(i * LANES, LANES), LANES)
        lane = c * cpb + i
        pad_g[n, rows:, :] = jnp.zeros((halo, LANES), F32)
        gains = jnp.zeros((8, LANES), F32)
        sums = [jnp.zeros((8, LANES), F32) for _ in range(taps_se)]

        def fold(value):
            return jnp.sum(value.reshape(-1, 8, LANES), axis=0)

        taps_of = [fse[c, j : j + 1, cols] for j in range(taps_se)]
        gain_of = gain[c, :, cols]
        for start in range(rows - high, -1, -high):
            at_rows = slice(start, start + high)
            back = normed[c, at_rows, cols] * scale[at_rows, :]
            quer = q[c, at_rows, cols].astype(F32)
            value = conv[c, at_rows, cols]
            mixed = quer * value
            gm = gain_of * back - mixed * coef[at_rows, :]
            gains = gains + fold(back * mixed)
            q[c, at_rows, cols] = (gm * value).astype(BF16)
            gc = (gm * quer).astype(BF16).astype(F32)
            pad_g[n, at_rows, :] = gc
            if start + high == rows:
                lasts[lane, :halo, :] = gc[high - halo :, :]
            gp = taps_of[0] * gc
            for j in range(taps_se):
                if j:
                    gp = gp + taps_of[j] * pad_g[n, pl.ds(start + j, high), :]
                sums[j] = sums[j] + fold(gc * prod[lane, pl.ds(start + halo - j, high), :])
            key = k[c, at_rows, cols].astype(F32)
            k[c, at_rows, cols] = (gp * v[c, at_rows, cols].astype(F32)).astype(BF16)
            v[c, at_rows, cols] = (gp * key).astype(BF16)
        part = lane * LANES // group
        place = pl.ds(pl.multiple_of(lax.rem(lane * LANES, group), LANES), LANES)
        for j, value in enumerate(sums + [gains]):
            small[part, j : j + 1, place] = jnp.sum(value, axis=0, keepdims=True)

    def bottom_step(c):
        for i in range(cpb):
            cols = slice(i * LANES, (i + 1) * LANES)
            lane = c * cpb + i
            at = pl.ds(pl.multiple_of(lane * LANES, LANES), LANES)
            lasts[lane, halo:, :] = received(head_in, c, i)
            gp = fse[c, 0:1, cols] * lasts[lane, :halo, :]
            for j in range(1, taps_se):
                gp = gp + fse[c, j : j + 1, cols] * lasts[lane, pl.ds(j, halo), :]
            for kept, other in ((k, ends[1, :, at]), (v, ends[0, :, at])):
                old = kept[c, rows - edge :, cols].astype(F32)
                new = gp * other.astype(F32)[edge - halo :]
                kept[c, rows - edge :, cols] = jnp.concatenate(
                    [old[: edge - halo], new], 0
                ).astype(BF16)

    def back_step(p):
        c, i = (p * lanes) // cpb, lax.rem(p * lanes, cpb)
        for n in range(lanes):
            back_lane(c, i + n, n)

    def swap(step):
        there = lax.rem(ctx + step, nctx)
        return remote(small.at[there], small_in.at[step - 1], swap_send.at[0],
                      swap_recv.at[0], {"ctx": there})

    def medium_step(cs):
        with jax.named_scope("p_wtail"):
            part = zfull.at[pl.ds(cs[0], batch), pl.ds(0, taps), :]
            pl.when(ctx > 0)(lambda: settle(part, tail_recv.at[cs[0] // batch]))
        found = [dot(fz[:, :taps], zfull[c, :taps, :]) for c in cs]
        mixes = []
        for c, value in zip(cs, found):
            zr, zi = zs[c, :half, :] + value[:half], zs[c, half:, :] + value[half:]
            hr, hi = hs[c, :half, :], hs[c, half:, :]
            mixes.append(spectrum_of(zr * hr - zi * hi, zr * hi + zi * hr))
        found = [dot(inv[:rows, :], mix) for mix in mixes]
        for c, value in zip(cs, found):
            up[c] = (up[c].astype(F32) * value).astype(BF16)

    per = nblk * cpb // lanes
    early = per * 3 // 4
    with jax.named_scope("p_back"):
        each(early, back_step)
    pass_on(1)
    with jax.named_scope("p_back"):
        each(per - early, back_step, early)
    if ratio == 1:
        for step in range(1, nctx):
            swap(step).start()
    with jax.named_scope("p_headse"):
        pl.when(ctx < nctx - 1)(head_se.wait_recv)
    with jax.named_scope("p_bottom"):
        each(nblk, bottom_step)
    with jax.named_scope("p_medium"):
        several(0, nblk, medium_step)
    for s in range(2, steps):
        pass_on(s)

    with jax.named_scope("p_swap"):
        total_o[...] = corr[mine] * factor
        if ratio == 1:
            value = small[mine]
            settle(small_in, swap_recv.at[0])
            for step in range(1, nctx):
                value = value + small_in[step - 1]
            small_o[...] = value * factor
        else:
            small_o[...] = small[...]

    with jax.named_scope("p_fin"):
        @pl.when(ctx > 0)
        def _():
            settle(gfull.at[:, pl.ds(0, taps), :], head_send.at[0])
            head_se.wait_send()

        @pl.when(ctx < nctx - 1)
        def _():
            settle(zfull.at[:, pl.ds(rows, taps), :], tail_send.at[0])
            tail_se.wait_send()

        for which in range(2):
            for step in range(1, ntp):
                row_copy(which, step).wait_send()
        for s in range(steps):
            halve_copy(s).wait_send()
        if ratio == 1:
            settle(small_in, swap_send.at[0])


def output_kernel(whole, *refs):
    count = 9 if whole else 5
    q, k, v, qm, up, total, small = refs[:7]
    outs, (sems,) = refs[7 : 7 + count], refs[7 + count :]
    gq_o, gk_o, gv_o, gqm_o, gkm_o = outs[:5]
    nblk, rows, blk = q.shape

    def copy(src, dst, s, c):
        at = pl.ds(pl.multiple_of(c * blk, blk), blk)
        return pltpu.make_async_copy(src.at[c], dst.at[:, at], sems.at[s])

    streams = ((q, gq_o), (k, gk_o), (v, gv_o), (qm, gkm_o), (up, gqm_o))

    def begin(c, carry):
        for s in range(5):
            copy(*streams[s], s, c).start()
        return carry

    lax.fori_loop(0, nblk, begin, 0)
    if whole:
        filter_se, filter_mr, skip, gain = outs[5:]
        taps_se = filter_se.shape[0]
        filter_se[...] = small[:taps_se, :]
        filter_mr[...] = total[...]
        skip[...] = total[0:1, :]
        gain[...] = small[taps_se : taps_se + 1, :]

    for s, (src, _) in enumerate(streams):
        pltpu.make_async_copy(src, src, sems.at[s]).wait()


def split_parts(parts, share):
    count, height, group = parts.shape
    if group == share:
        return parts
    parts = parts.reshape(count, height, group // share, share)
    return parts.transpose(0, 2, 1, 3).reshape(-1, height, share)


def scatter_sum(parts, axis, stop):
    size = lax.axis_size(axis)
    me = lax.axis_index(axis)
    bit = 1
    while bit < stop:
        rest = parts.reshape((parts.shape[0] // 2, 2) + parts.shape[1:])
        mine = lax.rem(me // bit, 2)
        away = lax.dynamic_index_in_dim(rest, 1 - mine, 1, keepdims=False).astype(BF16)
        keep = lax.dynamic_index_in_dim(rest, mine, 1, keepdims=False)
        with jax.named_scope(f"halve_{bit}"):
            got = lax.ppermute(away, axis, [(i, i ^ bit) for i in range(size)])
        parts = keep + got.astype(F32)
        bit *= 2
    return parts[0]


def local(
    query_se, key_se, value_se, query_mr, key_mr, upstream, filter_se, filter_mr, skip_mr, norm_gain
):
    rows, chans = query_se.shape
    taps_se, taps = filter_se.shape[0], filter_mr.shape[0]
    ctx, ntp = lax.axis_size("ctx"), lax.axis_size("tp")
    width = chans * ntp
    tokens = rows * ctx
    share = chans // ctx
    group = up_to(share, LANES)
    halo, edge = up_to(taps_se - 1, 8), up_to(taps_se - 1, 16)
    blk = max(group, min(512, chans // 2))
    nblk = chans // blk
    fz, fg, inv = transforms(rows, taps)
    length = rows + taps
    tall = up_to(rows, LANES)
    nlane = chans // LANES

    def out(shape, kind):
        return jax.ShapeDtypeStruct(shape, kind)

    ins = (query_se, key_se, value_se, query_mr, key_mr, upstream, filter_se, filter_mr,
           skip_mr[None], norm_gain[None], fg, fz, inv)
    V, D = pltpu.VMEM, pltpu.SemaphoreType.DMA
    ratio = group // share
    parts = chans // group
    small_height = taps_se + 1
    small_shape = (small_height, group) if ratio == 1 else (parts, small_height, group)
    stream = V((nblk, rows, blk), BF16)
    outs = [stream] * 5 + [V((taps, group), F32), V(small_shape, F32)]
    lanes = runs(blk // LANES)
    message = (2 * halo, chans // 2)
    steps = len(halving_bits(ctx, ratio))
    scratch = [
        stream, V((nblk, taps_se, blk), F32), V((nblk, taps, blk), F32), V((nblk, 1, blk), F32),
        V((nblk, 1, blk), F32), V(fg.shape, BF16), V(fz.shape, BF16), V(inv.shape, BF16),
        V((2, edge, chans), BF16), V(message, BF16), V(message, BF16), V(message, BF16),
        V(message, BF16),
        V((nblk, length, blk), BF16), V((nblk, length, blk), BF16),
        V((nblk, rows, blk), F32), V((nblk, rows, blk), F32),
        V((nblk, length, blk), F32), V((nblk, length, blk), F32),
        V((nlane, halo + rows, LANES), F32), V((lanes, halo + rows, LANES), F32),
        V((nlane, 2 * halo, LANES), F32),
        V((parts, taps, group), F32), V((parts, small_height, group), F32),
        V((parts, taps, group), BF16), V((parts, taps, group), BF16),
        V((max(ctx - 1, 1), small_height, group), F32),
        V((tall, LANES), F32), V((rows, LANES), F32), V((rows, LANES), F32),
        V((2, 8, tall), F32), V((2, max(ntp - 1, 1), 8, tall), F32),
        D((7,)), D((3,)), D((5,)), D((2,)), D((2,)),
        D((1,)), D((nblk // runs(nblk),)), D((1,)), D((nblk // runs(nblk),)),
        D((2, max(ntp - 1, 1))), D((2, max(ntp - 1, 1))),
        D((steps,)), D((steps,)), D((1,)), D((1,)),
    ]
    anywhere = pl.BlockSpec(memory_space=pl.ANY)
    inside = pl.BlockSpec(memory_space=pltpu.VMEM)
    with jax.named_scope("layer"):
        held = pl.pallas_call(
            functools.partial(layer_kernel, width, tokens, ctx, ntp, ratio),
            name="layer",
            in_specs=[anywhere] * len(ins),
            out_specs=[inside] * len(outs),
            out_shape=outs,
            scratch_shapes=scratch,
            compiler_params=pltpu.CompilerParams(
                collective_id=0, has_side_effects=True, vmem_limit_bytes=48 * 2**20
            ),
        )(*ins)

    def out(shape, kind):
        return jax.ShapeDtypeStruct(shape, kind)

    results = [out((rows, chans), BF16)] * 5
    specs = [anywhere] * 5
    if ratio == 1:
        results += [out((n, share), F32) for n in (taps_se, taps, 1, 1)]
        specs += [inside] * 4
    with jax.named_scope("output"):
        found = pl.pallas_call(
            functools.partial(output_kernel, ratio == 1),
            name="output",
            in_specs=[inside] * len(held),
            out_specs=specs,
            out_shape=results,
            scratch_shapes=[D((5,))],
            compiler_params=pltpu.CompilerParams(vmem_limit_bytes=8 * 2**20),
        )(*[pltpu.with_memory_space_constraint(a, pltpu.VMEM) for a in held])
    if ratio == 1:
        return (*found[:7], found[7].reshape(share), found[8].reshape(share))
    total_mr, small = held[5], held[6]
    total_mr = scatter_sum(split_parts(total_mr[None], share), "ctx", ratio)
    small = lax.all_to_all(split_parts(small, share), "ctx", 0, 0, tiled=True)
    total = jnp.sum(small, axis=0) * (1.0 / math.sqrt(tokens))
    return (*found, total[:taps_se], total_mr, total_mr[0], total[taps_se])


def solution(mesh):
    streams = (P("ctx", "tp"),)
    in_specs = streams * 6 + (P(None, "tp"), P(None, "tp"), P("tp"), P("tp"))
    both = ("tp", "ctx")
    out_specs = streams * 5 + (P(None, both), P(None, both), P(both), P(both))
    return jax.shard_map(local, mesh=mesh, in_specs=in_specs, out_specs=out_specs, check_vma=False)
```
